256 devices in a mesh: gz: 128 (over x_lo, y, z, core), gy: 2 (over x_hi).
Axes of the slice: x: 4 (x_hi: 2, x_lo: 2; x = x_hi * 2 + x_lo), y: 4, z: 8, core: 2. Of those that a mesh axis runs over, the one named last changes fastest.
Arguments:
- fixed_image: float32 [1280, 80, 320], P('gz', 'gy'), may hold values from -6 to 6
- moving_image: float32 [1280, 80, 320], P('gz', 'gy'), may hold values from -6 to 6
- moving_grad: float32 [3, 1280, 80, 320], P(None, 'gz', 'gy'), may hold values from -6 to 6
Outputs:
- control_grad: float32 [256, 3, 16, 64], P('gz', None, 'gy')
The draws below stay inside these ranges and needn't reach their ends.
All inputs are finite; a program needn't handle non-finite values.
Results may differ from the reference program's by a relative error of at most 0.00016.
Values sent between devices are 32-bit elements; how exact they have to be, the bound alone decides.
A program may use at most 64 MiB of HBM per device.

```python
import jax
import jax.numpy as jnp
from jax import lax

NX = 320
RADIUS = 4
SPACING = 5
NZ = 1280
NY = 80
CZ = 256
CY = 16
CX = 64


def block_levels(key, shape, split, smallest, top_value):
    level, own = 1.0, jax.random.fold_in(key, 6)
    for axis_at, shards_of in split:
        heights = jnp.exp(jax.random.uniform(jax.random.fold_in(own, axis_at), (shards_of,), jnp.float32, smallest / len(split), top_value / len(split)))
        level = level * jnp.repeat(heights, shape[axis_at] // shards_of).reshape([-1 if axis == axis_at else 1 for axis in range(len(shape))])
    return level


def bell_draw(rng, extent, scale, limit, cuts=(), held_as=jnp.bfloat16):
    factor_of = block_levels(rng, extent, cuts, -0.22, 0.18) if cuts else 1.0
    entries = jax.random.normal(rng, extent, jnp.float32) * scale * factor_of
    return jnp.minimum(jnp.maximum(entries, -limit), limit).astype(held_as)


def setup_inputs(seed: int = 0) -> dict:
    arg_keys = jax.random.split(jax.random.key(seed), 4)
    return {
        "fixed_image": bell_draw(arg_keys[0], (NZ, NY, NX), 1.0, 6.0, ((0, 128), (1, 2)), jnp.float32),
        "moving_image": bell_draw(arg_keys[1], (NZ, NY, NX), 1.0, 6.0, ((0, 128), (1, 2)), jnp.float32),
        "moving_grad": bell_draw(arg_keys[2], (3, NZ, NY, NX), 1.0, 6.0, ((1, 128), (2, 2)), jnp.float32),
    }


EPS = 36.0
SIM_WEIGHT = 8.0


def spline_basis(voxels, points, anchor, first_point, columns):
    position = anchor + jnp.arange(voxels, dtype=jnp.int32)
    cell_index = position // SPACING
    fraction = (position - cell_index * SPACING).astype(jnp.float32) / SPACING
    remainder = 1.0 - fraction
    weights = [remainder ** 3 / 6.0,
               (3.0 * fraction ** 3 - 6.0 * fraction ** 2 + 4.0) / 6.0,
               (-3.0 * fraction ** 3 + 3.0 * fraction ** 2 + 3.0 * fraction + 1.0) / 6.0,
               fraction ** 3 / 6.0]
    targets = first_point + jnp.arange(columns, dtype=jnp.int32)
    matrix = jnp.zeros((voxels, columns), jnp.float32)
    for spline in range(4):
        clamped = jnp.clip(cell_index - 1 + spline, 0, points - 1)
        matrix = matrix + weights[spline][:, None] * (clamped[:, None] == targets[None, :]).astype(jnp.float32)
    return matrix


def box_axis(values, dimension):
    length = values.shape[dimension]
    widths = [(0, 0)] * values.ndim
    widths[dimension] = (RADIUS, RADIUS)
    padded = jnp.pad(values, widths)
    running = lax.slice_in_dim(padded, 0, length, axis=dimension)
    for offset in range(1, 2 * RADIUS + 1):
        running = running + lax.slice_in_dim(padded, offset, offset + length, axis=dimension)
    return running


def box_full(values):
    return box_axis(box_axis(box_axis(values, 2), 1), 0)


def reference(fixed_image, moving_image, moving_grad):
    fixed_part = fixed_image.astype(jnp.float32)
    moving_part = moving_image.astype(jnp.float32)
    window_size = float((2 * RADIUS + 1) ** 3)
    sum_f = box_full(fixed_part)
    sum_m = box_full(moving_part)
    sum_ff = box_full(fixed_part * fixed_part)
    sum_mm = box_full(moving_part * moving_part)
    sum_fm = box_full(fixed_part * moving_part)
    covariance = sum_fm - sum_f * sum_m / window_size
    variance_fixed = sum_ff - sum_f * sum_f / window_size + EPS
    variance_moving = sum_mm - sum_m * sum_m / window_size + EPS
    quotient = covariance / (variance_fixed * variance_moving)
    weight_cross = 2.0 * quotient
    weight_moving = -quotient * covariance / variance_moving
    boxed_one = box_full(weight_cross)
    boxed_two = box_full(weight_cross * sum_f / window_size)
    boxed_three = box_full(weight_moving)
    boxed_four = box_full(weight_moving * sum_m / window_size)
    similarity_slope = -SIM_WEIGHT * (fixed_part * boxed_one - boxed_two + 2.0 * moving_part * boxed_three - 2.0 * boxed_four)
    basis_x = spline_basis(NX, CX, 0, 0, CX)
    basis_y = spline_basis(NY, CY, 0, 0, CY)
    basis_z = spline_basis(NZ, CZ, 0, 0, CZ)
    results = []
    for component in range(3):
        voxel_grad = similarity_slope * moving_grad[component].astype(jnp.float32)
        along_x = jnp.dot(voxel_grad.reshape(-1, NX), basis_x, precision=lax.Precision.HIGHEST).reshape(NZ, NY, CX)
        along_y = jnp.einsum("zyx,yb->zbx", along_x, basis_y, precision=lax.Precision.HIGHEST)
        results.append(jnp.einsum("zbx,zq->qbx", along_y, basis_z, precision=lax.Precision.HIGHEST))
    return jnp.stack(results, axis=1)
```

```python
import functools

import jax
import jax.numpy as jnp
import numpy as np
from jax import lax
from jax.experimental import pallas as pl
from jax.experimental.pallas import tpu as pltpu
from jax.sharding import PartitionSpec as P

RADIUS = 4
SPACING = 5
EPS = 36.0
SIM_WEIGHT = 8.0
WINDOW = float((2 * RADIUS + 1) ** 3)
MESH = pl.DeviceIdType.MESH

PLANES = 10
ROWS = 40
NX = 320
POINTS = 64
HALO = 2 * RADIUS
RAW_PLANES = PLANES + 2 * HALO
RAW_ROWS = ROWS + 2 * HALO
COEF_PLANES = PLANES + 2 * RADIUS
COEF_ROWS = ROWS + 2 * RADIUS
PAIRS = (0, 8, 2, 6, 4)


def spline_weights(step):
    u = step / SPACING
    return (
        (1.0 - u) ** 3 / 6.0,
        (3.0 * u**3 - 6.0 * u**2 + 4.0) / 6.0,
        (-3.0 * u**3 + 3.0 * u**2 + 3.0 * u + 1.0) / 6.0,
        u**3 / 6.0,
    )


def basis_along_x():
    matrix = np.zeros((384, 128), np.float64)
    for x in range(NX):
        for k, weight in enumerate(spline_weights(x % SPACING)):
            point = min(max(x // SPACING - 1 + k, 0), POINTS - 1)
            matrix[x, point] += weight
    matrix = matrix.astype(np.float32)
    high = matrix.astype(jnp.bfloat16)
    low = (matrix - high.astype(np.float32)).astype(jnp.bfloat16)
    return high, low


def suffix_sums(values):
    sums = [values[-1]]
    for value in reversed(values[:-1]):
        sums.append(sums[-1] + value)
    return sums[::-1]


def prefix_sums(values):
    sums = [values[0]]
    for value in values[1:]:
        sums.append(sums[-1] + value)
    return sums


def windows_of_nine(values):
    count = len(values) - 8
    if count > 9:
        before = suffix_sums(values[:9])
        after = prefix_sums(values[9:])
        return [before[0]] + [before[i] + after[i - 1] for i in range(1, 9)] + [after[8]]
    common = values[count - 1]
    for value in values[count:9]:
        common = common + value
    before = suffix_sums(values[: count - 1])
    after = prefix_sums(values[9:])
    out = []
    for i in range(count):
        total = common
        if i < count - 1:
            total = total + before[i]
        if i > 0:
            total = total + after[i - 1]
        out.append(total)
    return out


def box_along_x(tiles, lane):
    def shifted(parts, amount):
        turned = [pltpu.roll(part, amount % 128, 1) for part in parts]
        if amount > 0:
            return [jnp.where(lane < amount, turned[i - 1], turned[i]) for i in range(3)]
        return [jnp.where(lane >= 128 + amount, turned[(i + 1) % 3], turned[i]) for i in range(3)]

    three = [a + b + c for a, b, c in zip(tiles, shifted(tiles, 1), shifted(tiles, -1))]
    return [a + b + c for a, b, c in zip(three, shifted(three, 3), shifted(three, -3))]


def kernel(
    depth, f_hbm, m_hbm, g_hbm, bh_hbm, bl_hbm, out_ref,
    raw, f_tail, m_tail, grad, g_tail, bh, bl, own_sum, halo_sum, zsum, coef, zcoef, weighted, wide,
    sums, from_next, from_prev, from_side, from_next_side, from_prev_side,
    local_sem, y_send, y_recv, z_send, z_recv, s_send, s_recv, e_send, e_recv,
):
    gz = lax.axis_index("gz")
    gy = lax.axis_index("gy")
    other = 1 - gy
    is_first = gz == 0
    is_last = gz == depth - 1
    before = (jnp.maximum(gz - 1, 0), gy)
    after = (jnp.minimum(gz + 1, depth - 1), gy)
    before_side = (jnp.maximum(gz - 1, 0), other)
    after_side = (jnp.minimum(gz + 1, depth - 1), other)
    side = (gz, other)

    local = []

    def bring(src, dst):
        copy = pltpu.make_async_copy(src, dst, local_sem.at[len(local)])
        copy.start()
        local.append(copy)

    own = pl.ds(HALO, PLANES)
    rows_own = pl.ds(HALO, ROWS)
    bring(f_hbm.at[:, :, pl.ds(256, 64)], f_tail)
    bring(m_hbm.at[:, :, pl.ds(256, 64)], m_tail)
    for t in range(2):
        bring(f_hbm.at[:, :, pl.ds(128 * t, 128)], raw.at[t, own, rows_own, :])
        bring(m_hbm.at[:, :, pl.ds(128 * t, 128)], raw.at[2 + t, own, rows_own, :])
    for t in range(2):
        bring(g_hbm.at[:, :, :, pl.ds(128 * t, 128)], grad.at[t])
    bring(g_hbm.at[:, :, :, pl.ds(256, 64)], g_tail)
    bring(bh_hbm, bh)
    bring(bl_hbm, bl)

    barrier = pltpu.get_barrier_semaphore()
    pl.semaphore_signal(barrier, inc=1, device_id=side, device_id_type=MESH)

    @pl.when(jnp.logical_not(is_first))
    def _():
        pl.semaphore_signal(barrier, inc=1, device_id=before, device_id_type=MESH)
        pl.semaphore_signal(barrier, inc=1, device_id=before_side, device_id_type=MESH)

    @pl.when(jnp.logical_not(is_last))
    def _():
        pl.semaphore_signal(barrier, inc=1, device_id=after, device_id_type=MESH)
        pl.semaphore_signal(barrier, inc=1, device_id=after_side, device_id_type=MESH)

    lane = lax.broadcasted_iota(jnp.int32, (8, 128), 1)
    row = lax.broadcasted_iota(jnp.int32, (8, 128), 0)
    zero = jnp.zeros((8, 128), jnp.float32)
    low_half = lane < 64

    zero_row = pl.multiple_of(48 * gy, 8)
    strip_row = pl.multiple_of(48 - 48 * gy, 8)
    zsum[:, pl.ds(zero_row, 8), :] = jnp.zeros((26, 8, 128), jnp.float32)
    halo_sum[...] = jnp.zeros_like(halo_sum)

    local[0].wait()
    local[1].wait()
    for z in range(PLANES):
        raw[4, HALO + z, HALO : HALO + ROWS, :] = jnp.concatenate([f_tail[z], m_tail[z]], axis=-1)
    for copy in local[2:6]:
        copy.wait()

    @pl.when(is_first | is_last)
    def _():
        pl.semaphore_wait(barrier, 3)

    @pl.when(jnp.logical_not(is_first | is_last))
    def _():
        pl.semaphore_wait(barrier, 5)

    src_row = pl.multiple_of(40 - 32 * gy, 8)
    y_copies = []
    for i, first in enumerate(PAIRS):
        copy = pltpu.make_async_remote_copy(
            src_ref=raw.at[:, pl.ds(HALO + first, 2), pl.ds(src_row, 8), :],
            dst_ref=raw.at[:, pl.ds(HALO + first, 2), pl.ds(zero_row, 8), :],
            send_sem=y_send.at[i], recv_sem=y_recv.at[i], device_id=side, device_id_type=MESH,
        )
        copy.start()
        y_copies.append(copy)

    def to_after(k, rows, send, recv):
        return pltpu.make_async_remote_copy(
            src_ref=raw.at[:, pl.ds(16 - 2 * k, 2), rows, :],
            dst_ref=raw.at[:, pl.ds(6 - 2 * k, 2), rows, :],
            send_sem=send.at[0, k], recv_sem=recv.at[0, k], device_id=after, device_id_type=MESH,
        )

    def to_before(k, rows, send, recv):
        return pltpu.make_async_remote_copy(
            src_ref=raw.at[:, pl.ds(8 + 2 * k, 2), rows, :],
            dst_ref=raw.at[:, pl.ds(18 + 2 * k, 2), rows, :],
            send_sem=send.at[1, k], recv_sem=recv.at[1, k], device_id=before, device_id_type=MESH,
        )

    strip = pl.ds(strip_row, 8)

    def start_planes(k, rows, send, recv):
        @pl.when(jnp.logical_not(is_last))
        def _():
            to_after(k, rows, send, recv).start()

        @pl.when(jnp.logical_not(is_first))
        def _():
            to_before(k, rows, send, recv).start()

    def wait_planes(k, rows, send, recv):
        @pl.when(jnp.logical_not(is_first))
        def _():
            to_after(k, rows, send, recv).wait_recv()

        @pl.when(jnp.logical_not(is_last))
        def _():
            to_before(k, rows, send, recv).wait_recv()

    def wait_sent(k, rows, send, recv):
        @pl.when(jnp.logical_not(is_last))
        def _():
            to_after(k, rows, send, recv).wait_send()

        @pl.when(jnp.logical_not(is_first))
        def _():
            to_before(k, rows, send, recv).wait_send()

    for k in range(3):
        start_planes(k, rows_own, z_send, z_recv)

    @pl.when(is_first)
    def _():
        raw[:, 0:HALO, :, :] = jnp.zeros((5, HALO, RAW_ROWS, 128), jnp.float32)

    @pl.when(is_last)
    def _():
        raw[:, HALO + PLANES : RAW_PLANES, :, :] = jnp.zeros((5, HALO, RAW_ROWS, 128), jnp.float32)

    def fields_of(plane, rows):
        out = []
        for t in range(2):
            f = raw[t, plane, rows, :]
            m = raw[2 + t, plane, rows, :]
            out += [f, m, f * f, m * m, f * m]
        p = raw[4, plane, rows, :]
        return out + [p, p * p, p * pltpu.roll(p, 64, 1)]

    def own_windows(rows):
        columns = [fields_of(HALO + z, rows) for z in range(PLANES)]
        for col in range(13):
            values = [columns[z][col] for z in range(PLANES)]
            for p, total in enumerate(prefix_sums(values[:9])):
                own_sum[col, p, rows, :] = total
            for p, total in enumerate(suffix_sums(values[1:])):
                own_sum[col, 9 + p, rows, :] = total

    @pl.loop(0, 5)
    def _(i):
        own_windows(pl.ds(pl.multiple_of(8 + 8 * i, 8), 8))

    y_copies[0].wait_recv()
    y_copies[1].wait_recv()
    start_planes(0, strip, s_send, s_recv)
    start_planes(3, rows_own, z_send, z_recv)
    y_copies[2].wait_recv()
    y_copies[3].wait_recv()
    start_planes(1, strip, s_send, s_recv)
    y_copies[4].wait_recv()
    start_planes(2, strip, s_send, s_recv)
    start_planes(3, strip, s_send, s_recv)
    own_windows(strip)

    row_valid = []
    for j in range(6):
        position = 6 * row + j + 40 * gy - 4
        row_valid.append(jnp.where((position >= 0) & (position < 80), 1.0, 0.0))

    groups = [pl.ds(8 + 8 * i, 8) for i in range(5)] + [strip]

    def coefficients(planes, halo):
        for s in range(2):
            for rows in groups:
                if halo is None:
                    for col in range(13):
                        zsum[13 * s + col, rows, :] = own_sum[col, planes[s], rows, :]
                else:
                    fields = fields_of(halo[s], rows)
                    for col in range(13):
                        total = halo_sum[s, col, rows, :] + fields[col]
                        halo_sum[s, col, rows, :] = total
                        zsum[13 * s + col, rows, :] = total + own_sum[col, planes[s], rows, :]
        for s in range(2):
            position = gz * PLANES + planes[s] - RADIUS
            inside = jnp.where((position >= 0) & (position < depth * PLANES), 1.0, 0.0)
            summed = []
            for col in range(13):
                summed.append(windows_of_nine([zsum[13 * s + col, pl.ds(m, 8, stride=6), :] for m in range(14)]))
            for j in range(6):
                v = [summed[col][j] for col in range(13)]
                tail, square = pltpu.roll(v[10], 64, 1), pltpu.roll(v[11], 64, 1)
                last = [jnp.where(low_half, a, 0.0) for a in (v[10], tail, v[11], square, v[12])]
                boxed = [box_along_x([v[i], v[5 + i], last[i]], lane) for i in range(5)]
                valid = row_valid[j] * inside
                for t in range(3):
                    sf, sm, sff, smm, sfm = [boxed[i][t] for i in range(5)]
                    mf = sf * (1.0 / WINDOW)
                    mm = sm * (1.0 / WINDOW)
                    a = (sfm - mf * sm) * (valid if t < 2 else jnp.where(low_half, valid, 0.0))
                    p = sff - mf * sf + EPS
                    q = smm - mm * sm + EPS
                    r = 1.0 / (p * q)
                    cross = a * r
                    moving = -cross * a * (r * p)
                    where = pl.ds(j, 8, stride=6)
                    coef[t, planes[s], where, :] = cross
                    coef[3 + t, planes[s], where, :] = moving
                    coef[6 + t, planes[s], where, :] = cross * mf + moving * mm

    coefficients((8, 9), None)

    @pl.loop(0, 4)
    def _(k):
        wait_planes(k, rows_own, z_send, z_recv)
        wait_planes(k, strip, s_send, s_recv)

        @pl.loop(0, 2)
        def _(half):
            step = 2 * k + half
            coefficients((7 - step, 10 + step), (7 - step, 18 + step))

    for copy in local[6:]:
        copy.wait()
    grad[2] = jnp.concatenate([g_tail[...], jnp.zeros_like(g_tail)], axis=-1)

    @pl.loop(0, 9)
    def _(col):
        for g in range(6):
            rows = pl.ds(8 * g, 8)
            for z, total in enumerate(windows_of_nine([coef[col, p, rows, :] for p in range(COEF_PLANES)])):
                zcoef[col, z, rows, :] = total

    def slope_plane(z):
        summed = []
        for col in range(9):
            summed.append(windows_of_nine([zcoef[col, z, pl.ds(m, 8, stride=5), :] for m in range(13)]))
        for j in range(5):
            boxed = [box_along_x([summed[3 * i + t][j] for t in range(3)], lane) for i in range(3)]
            centre = pl.ds(HALO + j, 8, stride=5)
            tail = raw[4, HALO + z, centre, :]
            f = [raw[0, HALO + z, centre, :], raw[1, HALO + z, centre, :], tail]
            m = [raw[2, HALO + z, centre, :], raw[3, HALO + z, centre, :], pltpu.roll(tail, 64, 1)]
            for t in range(3):
                slope = f[t] * boxed[0][t] + m[t] * boxed[1][t] - boxed[2][t]
                for c in range(3):
                    weighted[c, t, j, z] = slope * grad[t, c, z, pl.ds(j, 8, stride=5), :]

    @pl.loop(0, 5)
    def _(z):
        slope_plane(z)
        slope_plane(z + 5)

    wy = [spline_weights(j) for j in range(SPACING)]
    wz = [[-2.0 * SIM_WEIGHT * w for w in ws] for ws in wy]
    for t in range(3):
        @pl.loop(0, 3)
        def _(c):
            slots = []
            for j in range(SPACING):
                v = [weighted[c, t, j, z] for z in range(PLANES)]
                part = []
                for i in range(2):
                    for k in range(4):
                        total = wz[0][k] * v[5 * i]
                        for step in range(1, SPACING):
                            if wz[step][k] != 0.0:
                                total = total + wz[step][k] * v[5 * i + step]
                        part.append(total)
                slots.append([part[0], part[1] + part[4], part[2] + part[5], part[3] + part[6], part[7]])
            for m in range(5):
                y = []
                for k in range(4):
                    total = wy[0][k] * slots[0][m]
                    for j in range(1, SPACING):
                        total = total + wy[j][k] * slots[j][m]
                    y.append(total)
                r0, r2, r3 = pltpu.roll(y[0], 7, 0), pltpu.roll(y[2], 1, 0), pltpu.roll(y[3], 2, 0)
                inner = (
                    jnp.where(row == 7, 0.0, r0) + y[1] + jnp.where(row == 0, 0.0, r2) + jnp.where(row < 2, 0.0, r3)
                )
                to_low = jnp.where(row == 7, r0, 0.0)
                to_high = jnp.where(row == 0, r2, 0.0) + jnp.where(row < 2, r3, 0.0)
                clip_low = jnp.where(row == 0, y[0], 0.0)
                clip_high = jnp.where(row == 7, y[2] + y[3] + pltpu.roll(y[3], 1, 0), 0.0)
                is_low = gy == 0
                base = pl.multiple_of(48 * m + 8 * c, 8)
                lanes = pl.ds(128 * t, 128)
                wide[pl.ds(base, 8), lanes] = inner + jnp.where(is_low, clip_low, clip_high)
                wide[pl.ds(pl.multiple_of(base + 24, 8), 8), lanes] = jnp.where(is_low, to_high, to_low)

    left = wide[...]
    high = left.astype(jnp.bfloat16)
    low = (left - high.astype(jnp.float32)).astype(jnp.bfloat16)

    def dot(a, b):
        return jnp.dot(a, b, preferred_element_type=jnp.float32)

    total = dot(high, bh[...]) + (dot(low, bh[...]) + dot(high, bl[...]))
    sums[...] = total.reshape(5, 2, 3, 8, 128)

    copies = [
        (0, sums.at[0, 0], from_next, before, 0),
        (0, sums.at[0, 1], from_next_side, before_side, 1),
        (1, sums.at[pl.ds(3, 2), 0], from_prev, after, 2),
        (1, sums.at[pl.ds(3, 2), 1], from_prev_side, after_side, 3),
    ]
    rdmas = [
        (
            direction,
            pltpu.make_async_remote_copy(
                src_ref=src, dst_ref=dst, send_sem=e_send.at[i], recv_sem=e_recv.at[i],
                device_id=target, device_id_type=MESH,
            ),
        )
        for direction, src, dst, target, i in copies
    ]
    side_copy = pltpu.make_async_remote_copy(
        src_ref=sums.at[pl.ds(1, 2), 1], dst_ref=from_side, send_sem=e_send.at[4], recv_sem=e_recv.at[4],
        device_id=side, device_id_type=MESH,
    )

    @pl.when(jnp.logical_not(is_first))
    def _():
        for direction, copy in rdmas:
            if direction == 0:
                copy.start()

    @pl.when(jnp.logical_not(is_last))
    def _():
        for direction, copy in rdmas:
            if direction == 1:
                copy.start()

    low_clip = jnp.where(is_first, 1.0, 0.0)
    high_clip = jnp.where(is_last, 1.0, 0.0)
    sums[1] = sums[1] + low_clip * sums[0]
    sums[2] = sums[2] + high_clip * (sums[3] + sums[4])
    side_copy.start()

    @pl.when(is_last)
    def _():
        from_next[...] = jnp.zeros_like(from_next)
        from_next_side[...] = jnp.zeros_like(from_next_side)

    @pl.when(is_first)
    def _():
        from_prev[...] = jnp.zeros_like(from_prev)
        from_prev_side[...] = jnp.zeros_like(from_prev_side)

    @pl.when(jnp.logical_not(is_last))
    def _():
        for direction, copy in rdmas:
            if direction == 0:
                copy.wait_recv()

    @pl.when(jnp.logical_not(is_first))
    def _():
        for direction, copy in rdmas:
            if direction == 1:
                copy.wait_recv()

    side_copy.wait_recv()
    first = sums[1, 0] + from_side[0] + from_prev[0] + from_prev_side[0]
    second = sums[2, 0] + from_side[1] + from_prev[1] + from_prev_side[1] + from_next[...] + from_next_side[...]
    out_ref[0] = first[:, :, :POINTS]
    out_ref[1] = second[:, :, :POINTS]

    for copy in y_copies:
        copy.wait_send()
    for k in range(4):
        wait_sent(k, rows_own, z_send, z_recv)
        wait_sent(k, strip, s_send, s_recv)
    side_copy.wait_send()

    @pl.when(jnp.logical_not(is_first))
    def _():
        for direction, copy in rdmas:
            if direction == 0:
                copy.wait_send()

    @pl.when(jnp.logical_not(is_last))
    def _():
        for direction, copy in rdmas:
            if direction == 1:
                copy.wait_send()


def local_gradient(depth, fixed_image, moving_image, moving_grad):
    high, low = basis_along_x()
    f32 = jnp.float32
    anywhere = pl.BlockSpec(memory_space=pl.ANY)
    dma = pltpu.SemaphoreType.DMA
    return pl.pallas_call(
        functools.partial(kernel, depth),
        out_shape=jax.ShapeDtypeStruct((2, 3, 8, POINTS), f32),
        in_specs=[anywhere] * 5,
        out_specs=pl.BlockSpec(memory_space=pltpu.VMEM),
        scratch_shapes=[
            pltpu.VMEM((5, RAW_PLANES, RAW_ROWS, 128), f32),
            pltpu.VMEM((PLANES, ROWS, 64), f32),
            pltpu.VMEM((PLANES, ROWS, 64), f32),
            pltpu.VMEM((3, 3, PLANES, ROWS, 128), f32),
            pltpu.VMEM((3, PLANES, ROWS, 64), f32),
            pltpu.VMEM((384, 128), jnp.bfloat16),
            pltpu.VMEM((384, 128), jnp.bfloat16),
            pltpu.VMEM((13, COEF_PLANES, RAW_ROWS, 128), f32),
            pltpu.VMEM((2, 13, RAW_ROWS, 128), f32),
            pltpu.VMEM((26, RAW_ROWS, 128), f32),
            pltpu.VMEM((9, COEF_PLANES, COEF_ROWS, 128), f32),
            pltpu.VMEM((9, PLANES, COEF_ROWS, 128), f32),
            pltpu.VMEM((3, 3, 5, PLANES, 8, 128), f32),
            pltpu.VMEM((240, 384), f32),
            pltpu.VMEM((5, 2, 3, 8, 128), f32),
            pltpu.VMEM((3, 8, 128), f32),
            pltpu.VMEM((2, 3, 8, 128), f32),
            pltpu.VMEM((2, 3, 8, 128), f32),
            pltpu.VMEM((3, 8, 128), f32),
            pltpu.VMEM((2, 3, 8, 128), f32),
            dma((11,)),
            dma((5,)),
            dma((5,)),
            dma((2, 4)),
            dma((2, 4)),
            dma((2, 4)),
            dma((2, 4)),
            dma((5,)),
            dma((5,)),
        ],
        compiler_params=pltpu.CompilerParams(collective_id=0, has_side_effects=True, vmem_limit_bytes=60 * 1024 * 1024),
    )(fixed_image, moving_image, moving_grad, high, low)


def solution(mesh):
    in_specs = (P("gz", "gy", None), P("gz", "gy", None), P(None, "gz", "gy", None))
    out_specs = P("gz", None, "gy", None)
    body = functools.partial(local_gradient, mesh.shape["gz"])
    return jax.shard_map(body, mesh=mesh, in_specs=in_specs, out_specs=out_specs, check_vma=False)
```

```python
import functools

import jax
import jax.numpy as jnp
import numpy as np
from jax import lax
from jax.experimental import pallas as pl
from jax.experimental.pallas import tpu as pltpu
from jax.sharding import PartitionSpec as P

RADIUS = 4
SPACING = 5
EPS = 36.0
SIM_WEIGHT = 8.0
WINDOW = float((2 * RADIUS + 1) ** 3)
MESH = pl.DeviceIdType.MESH

PLANES = 10
ROWS = 40
NX = 320
POINTS = 64
HALO = 2 * RADIUS
RAW_PLANES = PLANES + 2 * HALO
RAW_ROWS = ROWS + 2 * HALO
COEF_PLANES = PLANES + 2 * RADIUS
COEF_ROWS = ROWS + 2 * RADIUS
PAIRS = (0, 8, 2, 6, 4)


def spline_weights(step):
    u = step / SPACING
    return (
        (1.0 - u) ** 3 / 6.0,
        (3.0 * u**3 - 6.0 * u**2 + 4.0) / 6.0,
        (-3.0 * u**3 + 3.0 * u**2 + 3.0 * u + 1.0) / 6.0,
        u**3 / 6.0,
    )


def basis_along_x():
    matrix = np.zeros((384, 128), np.float64)
    for x in range(NX):
        for k, weight in enumerate(spline_weights(x % SPACING)):
            point = min(max(x // SPACING - 1 + k, 0), POINTS - 1)
            matrix[x, point] += weight
    matrix = matrix.astype(np.float32)
    high = matrix.astype(jnp.bfloat16)
    low = (matrix - high.astype(np.float32)).astype(jnp.bfloat16)
    return high, low


def suffix_sums(values):
    sums = [values[-1]]
    for value in reversed(values[:-1]):
        sums.append(sums[-1] + value)
    return sums[::-1]


def prefix_sums(values):
    sums = [values[0]]
    for value in values[1:]:
        sums.append(sums[-1] + value)
    return sums


def windows_of_nine(values):
    count = len(values) - 8
    if count > 9:
        before = suffix_sums(values[:9])
        after = prefix_sums(values[9:])
        return [before[0]] + [before[i] + after[i - 1] for i in range(1, 9)] + [after[8]]
    common = values[count - 1]
    for value in values[count:9]:
        common = common + value
    before = suffix_sums(values[: count - 1])
    after = prefix_sums(values[9:])
    out = []
    for i in range(count):
        total = common
        if i < count - 1:
            total = total + before[i]
        if i > 0:
            total = total + after[i - 1]
        out.append(total)
    return out


def three_along_x(tiles, reach, lane):
    right = [pltpu.roll(tile, reach, 1) for tile in tiles]
    left = [pltpu.roll(tile, 128 - reach, 1) for tile in tiles]
    out = []
    for i in range(3):
        before = jnp.where(lane < reach, right[i - 1], right[i])
        after = jnp.where(lane >= 128 - reach, left[(i + 1) % 3], left[i])
        out.append(tiles[i] + before + after)
    return out


def kernel(
    depth, f_hbm, m_hbm, g_hbm, bh_hbm, bl_hbm, out_ref,
    raw, f_tail, m_tail, grad, g_tail, bh, bl, own_sum, halo_sum, zsum, stage_y, stage_x, coef, zcoef, weighted, wide,
    sums, from_next, from_prev, from_side, from_next_side, from_prev_side,
    local_sem, y_send, y_recv, z_send, z_recv, s_send, s_recv, e_send, e_recv,
):
    gz = lax.axis_index("gz")
    gy = lax.axis_index("gy")
    other = 1 - gy
    is_first = gz == 0
    is_last = gz == depth - 1
    before = (jnp.maximum(gz - 1, 0), gy)
    after = (jnp.minimum(gz + 1, depth - 1), gy)
    before_side = (jnp.maximum(gz - 1, 0), other)
    after_side = (jnp.minimum(gz + 1, depth - 1), other)
    side = (gz, other)

    local = []

    def bring(src, dst):
        copy = pltpu.make_async_copy(src, dst, local_sem.at[len(local)])
        copy.start()
        local.append(copy)

    own = pl.ds(HALO, PLANES)
    rows_own = pl.ds(HALO, ROWS)
    bring(f_hbm.at[:, :, pl.ds(256, 64)], f_tail)
    bring(m_hbm.at[:, :, pl.ds(256, 64)], m_tail)
    for t in range(2):
        bring(f_hbm.at[:, :, pl.ds(128 * t, 128)], raw.at[t, own, rows_own, :])
        bring(m_hbm.at[:, :, pl.ds(128 * t, 128)], raw.at[2 + t, own, rows_own, :])
    for t in range(2):
        bring(g_hbm.at[:, :, :, pl.ds(128 * t, 128)], grad.at[t])
    bring(g_hbm.at[:, :, :, pl.ds(256, 64)], g_tail)
    bring(bh_hbm, bh)
    bring(bl_hbm, bl)

    barrier = pltpu.get_barrier_semaphore()
    pl.semaphore_signal(barrier, inc=1, device_id=side, device_id_type=MESH)

    @pl.when(jnp.logical_not(is_first))
    def _():
        pl.semaphore_signal(barrier, inc=1, device_id=before, device_id_type=MESH)
        pl.semaphore_signal(barrier, inc=1, device_id=before_side, device_id_type=MESH)

    @pl.when(jnp.logical_not(is_last))
    def _():
        pl.semaphore_signal(barrier, inc=1, device_id=after, device_id_type=MESH)
        pl.semaphore_signal(barrier, inc=1, device_id=after_side, device_id_type=MESH)

    lane = lax.broadcasted_iota(jnp.int32, (8, 128), 1)
    row = lax.broadcasted_iota(jnp.int32, (8, 128), 0)
    zero = jnp.zeros((8, 128), jnp.float32)
    low_half = lane < 64

    zero_row = pl.multiple_of(48 * gy, 8)
    strip_row = pl.multiple_of(48 - 48 * gy, 8)
    zsum[:, pl.ds(zero_row, 8), :] = jnp.zeros((26, 8, 128), jnp.float32)
    halo_sum[...] = jnp.zeros_like(halo_sum)

    local[0].wait()
    local[1].wait()
    for z in range(PLANES):
        raw[4, HALO + z, HALO : HALO + ROWS, :] = jnp.concatenate([f_tail[z], m_tail[z]], axis=-1)
    for copy in local[2:6]:
        copy.wait()

    @pl.when(is_first | is_last)
    def _():
        pl.semaphore_wait(barrier, 3)

    @pl.when(jnp.logical_not(is_first | is_last))
    def _():
        pl.semaphore_wait(barrier, 5)

    src_row = pl.multiple_of(40 - 32 * gy, 8)
    y_copies = []
    for i, first in enumerate(PAIRS):
        copy = pltpu.make_async_remote_copy(
            src_ref=raw.at[:, pl.ds(HALO + first, 2), pl.ds(src_row, 8), :],
            dst_ref=raw.at[:, pl.ds(HALO + first, 2), pl.ds(zero_row, 8), :],
            send_sem=y_send.at[i], recv_sem=y_recv.at[i], device_id=side, device_id_type=MESH,
        )
        copy.start()
        y_copies.append(copy)

    def to_after(k, rows, send, recv):
        return pltpu.make_async_remote_copy(
            src_ref=raw.at[:, pl.ds(16 - 2 * k, 2), rows, :],
            dst_ref=raw.at[:, pl.ds(6 - 2 * k, 2), rows, :],
            send_sem=send.at[0, k], recv_sem=recv.at[0, k], device_id=after, device_id_type=MESH,
        )

    def to_before(k, rows, send, recv):
        return pltpu.make_async_remote_copy(
            src_ref=raw.at[:, pl.ds(8 + 2 * k, 2), rows, :],
            dst_ref=raw.at[:, pl.ds(18 + 2 * k, 2), rows, :],
            send_sem=send.at[1, k], recv_sem=recv.at[1, k], device_id=before, device_id_type=MESH,
        )

    strip = pl.ds(strip_row, 8)

    def start_planes(k, rows, send, recv):
        @pl.when(jnp.logical_not(is_last))
        def _():
            to_after(k, rows, send, recv).start()

        @pl.when(jnp.logical_not(is_first))
        def _():
            to_before(k, rows, send, recv).start()

    def wait_planes(k, rows, send, recv):
        @pl.when(jnp.logical_not(is_first))
        def _():
            to_after(k, rows, send, recv).wait_recv()

        @pl.when(jnp.logical_not(is_last))
        def _():
            to_before(k, rows, send, recv).wait_recv()

    def wait_sent(k, rows, send, recv):
        @pl.when(jnp.logical_not(is_last))
        def _():
            to_after(k, rows, send, recv).wait_send()

        @pl.when(jnp.logical_not(is_first))
        def _():
            to_before(k, rows, send, recv).wait_send()

    for k in range(3):
        start_planes(k, rows_own, z_send, z_recv)

    @pl.when(is_first)
    def _():
        raw[:, 0:HALO, :, :] = jnp.zeros((5, HALO, RAW_ROWS, 128), jnp.float32)

    @pl.when(is_last)
    def _():
        raw[:, HALO + PLANES : RAW_PLANES, :, :] = jnp.zeros((5, HALO, RAW_ROWS, 128), jnp.float32)

    def fields_of(plane, rows):
        out = []
        for t in range(2):
            f = raw[t, plane, rows, :]
            m = raw[2 + t, plane, rows, :]
            out += [f, m, f * f, m * m, f * m]
        p = raw[4, plane, rows, :]
        return out + [p, p * p, p * pltpu.roll(p, 64, 1)]

    def own_windows(rows):
        columns = [fields_of(HALO + z, rows) for z in range(PLANES)]
        for col in range(13):
            values = [columns[z][col] for z in range(PLANES)]
            for p, total in enumerate(prefix_sums(values[:9])):
                own_sum[col, p, rows, :] = total
            for p, total in enumerate(suffix_sums(values[1:])):
                own_sum[col, 9 + p, rows, :] = total

    @pl.loop(0, 5)
    def _(i):
        own_windows(pl.ds(pl.multiple_of(8 + 8 * i, 8), 8))

    y_copies[0].wait_recv()
    y_copies[1].wait_recv()
    start_planes(0, strip, s_send, s_recv)
    start_planes(3, rows_own, z_send, z_recv)
    y_copies[2].wait_recv()
    y_copies[3].wait_recv()
    start_planes(1, strip, s_send, s_recv)
    y_copies[4].wait_recv()
    start_planes(2, strip, s_send, s_recv)
    start_planes(3, strip, s_send, s_recv)
    own_windows(strip)

    row_valid = []
    for j in range(6):
        position = 6 * row + j + 40 * gy - 4
        row_valid.append(jnp.where((position >= 0) & (position < 80), 1.0, 0.0))

    groups = [pl.ds(8 + 8 * i, 8) for i in range(5)] + [strip]

    def coefficients(planes, halo):
        for s in range(2):
            for rows in groups:
                if halo is None:
                    for col in range(13):
                        zsum[13 * s + col, rows, :] = own_sum[col, planes[s], rows, :]
                else:
                    fields = fields_of(halo[s], rows)
                    for col in range(13):
                        total = halo_sum[s, col, rows, :] + fields[col]
                        halo_sum[s, col, rows, :] = total
                        zsum[13 * s + col, rows, :] = total + own_sum[col, planes[s], rows, :]
        for s in range(2):
            for col in range(13):
                total = windows_of_nine([zsum[13 * s + col, pl.ds(m, 8, stride=6), :] for m in range(14)])
                for j in range(6):
                    if col < 10:
                        stage_y[s, j, 3 * (col % 5) + col // 5] = total[j]
                    elif col == 12:
                        stage_y[s, j, 14] = jnp.where(low_half, total[j], 0.0)
                    else:
                        stage_y[s, j, 6 * (col - 10) + 2] = jnp.where(low_half, total[j], 0.0)
                        stage_y[s, j, 6 * (col - 10) + 5] = jnp.where(low_half, pltpu.roll(total[j], 64, 1), 0.0)
        for s in range(2):
            for j in range(6):
                for i in range(5):
                    three = three_along_x([stage_y[s, j, 3 * i + t] for t in range(3)], 1, lane)
                    for t in range(3):
                        stage_x[s, j, 3 * i + t] = three[t]
        for s in range(2):
            position = gz * PLANES + planes[s] - RADIUS
            inside = jnp.where((position >= 0) & (position < depth * PLANES), 1.0, 0.0)
            for j in range(6):
                boxed = [three_along_x([stage_x[s, j, 3 * i + t] for t in range(3)], 3, lane) for i in range(5)]
                valid = row_valid[j] * inside
                for t in range(3):
                    sf, sm, sff, smm, sfm = [boxed[i][t] for i in range(5)]
                    mf = sf * (1.0 / WINDOW)
                    mm = sm * (1.0 / WINDOW)
                    a = (sfm - mf * sm) * (valid if t < 2 else jnp.where(low_half, valid, 0.0))
                    p = sff - mf * sf + EPS
                    q = smm - mm * sm + EPS
                    r = 1.0 / (p * q)
                    cross = a * r
                    moving = -cross * a * (r * p)
                    where = pl.ds(j, 8, stride=6)
                    coef[t, planes[s], where, :] = cross
                    coef[3 + t, planes[s], where, :] = moving
                    coef[6 + t, planes[s], where, :] = cross * mf + moving * mm

    coefficients((8, 9), None)

    @pl.loop(0, 4)
    def _(k):
        wait_planes(k, rows_own, z_send, z_recv)
        wait_planes(k, strip, s_send, s_recv)

        @pl.loop(0, 2)
        def _(half):
            step = 2 * k + half
            coefficients((7 - step, 10 + step), (7 - step, 18 + step))

    for copy in local[6:]:
        copy.wait()
    grad[2] = jnp.concatenate([g_tail[...], jnp.zeros_like(g_tail)], axis=-1)

    @pl.loop(0, 9)
    def _(col):
        for g in range(6):
            rows = pl.ds(8 * g, 8)
            for z, total in enumerate(windows_of_nine([coef[col, p, rows, :] for p in range(COEF_PLANES)])):
                zcoef[col, z, rows, :] = total

    def slope_planes(planes):
        for s, z in enumerate(planes):
            for col in range(9):
                total = windows_of_nine([zcoef[col, z, pl.ds(m, 8, stride=5), :] for m in range(13)])
                for j in range(5):
                    stage_y[s, j, col] = total[j]
        for s in range(2):
            for j in range(5):
                for i in range(3):
                    three = three_along_x([stage_y[s, j, 3 * i + t] for t in range(3)], 1, lane)
                    for t in range(3):
                        stage_x[s, j, 3 * i + t] = three[t]
        for s, z in enumerate(planes):
            for j in range(5):
                boxed = [three_along_x([stage_x[s, j, 3 * i + t] for t in range(3)], 3, lane) for i in range(3)]
                centre = pl.ds(HALO + j, 8, stride=5)
                tail = raw[4, HALO + z, centre, :]
                f = [raw[0, HALO + z, centre, :], raw[1, HALO + z, centre, :], tail]
                m = [raw[2, HALO + z, centre, :], raw[3, HALO + z, centre, :], pltpu.roll(tail, 64, 1)]
                for t in range(3):
                    slope = f[t] * boxed[0][t] + m[t] * boxed[1][t] - boxed[2][t]
                    for c in range(3):
                        weighted[c, t, j, z] = slope * grad[t, c, z, pl.ds(j, 8, stride=5), :]

    @pl.loop(0, 5)
    def _(z):
        slope_planes((z, z + 5))

    wy = [spline_weights(j) for j in range(SPACING)]
    wz = [[-2.0 * SIM_WEIGHT * w for w in ws] for ws in wy]
    for t in range(3):
        @pl.loop(0, 3)
        def _(c):
            slots = []
            for j in range(SPACING):
                v = [weighted[c, t, j, z] for z in range(PLANES)]
                part = []
                for i in range(2):
                    for k in range(4):
                        total = wz[0][k] * v[5 * i]
                        for step in range(1, SPACING):
                            if wz[step][k] != 0.0:
                                total = total + wz[step][k] * v[5 * i + step]
                        part.append(total)
                slots.append([part[0], part[1] + part[4], part[2] + part[5], part[3] + part[6], part[7]])
            for m in range(5):
                y = []
                for k in range(4):
                    total = wy[0][k] * slots[0][m]
                    for j in range(1, SPACING):
                        total = total + wy[j][k] * slots[j][m]
                    y.append(total)
                r0, r2, r3 = pltpu.roll(y[0], 7, 0), pltpu.roll(y[2], 1, 0), pltpu.roll(y[3], 2, 0)
                inner = (
                    jnp.where(row == 7, 0.0, r0) + y[1] + jnp.where(row == 0, 0.0, r2) + jnp.where(row < 2, 0.0, r3)
                )
                to_low = jnp.where(row == 7, r0, 0.0)
                to_high = jnp.where(row == 0, r2, 0.0) + jnp.where(row < 2, r3, 0.0)
                clip_low = jnp.where(row == 0, y[0], 0.0)
                clip_high = jnp.where(row == 7, y[2] + y[3] + pltpu.roll(y[3], 1, 0), 0.0)
                is_low = gy == 0
                base = pl.multiple_of(48 * m + 8 * c, 8)
                lanes = pl.ds(128 * t, 128)
                wide[pl.ds(base, 8), lanes] = inner + jnp.where(is_low, clip_low, clip_high)
                wide[pl.ds(pl.multiple_of(base + 24, 8), 8), lanes] = jnp.where(is_low, to_high, to_low)

    left = wide[...]
    high = left.astype(jnp.bfloat16)
    low = (left - high.astype(jnp.float32)).astype(jnp.bfloat16)

    def dot(a, b):
        return jnp.dot(a, b, preferred_element_type=jnp.float32)

    total = dot(high, bh[...]) + (dot(low, bh[...]) + dot(high, bl[...]))
    sums[...] = total.reshape(5, 2, 3, 8, 128)

    copies = [
        (0, sums.at[0, 0], from_next, before, 0),
        (0, sums.at[0, 1], from_next_side, before_side, 1),
        (1, sums.at[pl.ds(3, 2), 0], from_prev, after, 2),
        (1, sums.at[pl.ds(3, 2), 1], from_prev_side, after_side, 3),
    ]
    rdmas = [
        (
            direction,
            pltpu.make_async_remote_copy(
                src_ref=src, dst_ref=dst, send_sem=e_send.at[i], recv_sem=e_recv.at[i],
                device_id=target, device_id_type=MESH,
            ),
        )
        for direction, src, dst, target, i in copies
    ]
    side_copy = pltpu.make_async_remote_copy(
        src_ref=sums.at[pl.ds(1, 2), 1], dst_ref=from_side, send_sem=e_send.at[4], recv_sem=e_recv.at[4],
        device_id=side, device_id_type=MESH,
    )

    @pl.when(jnp.logical_not(is_first))
    def _():
        for direction, copy in rdmas:
            if direction == 0:
                copy.start()

    @pl.when(jnp.logical_not(is_last))
    def _():
        for direction, copy in rdmas:
            if direction == 1:
                copy.start()

    low_clip = jnp.where(is_first, 1.0, 0.0)
    high_clip = jnp.where(is_last, 1.0, 0.0)
    sums[1] = sums[1] + low_clip * sums[0]
    sums[2] = sums[2] + high_clip * (sums[3] + sums[4])
    side_copy.start()

    @pl.when(is_last)
    def _():
        from_next[...] = jnp.zeros_like(from_next)
        from_next_side[...] = jnp.zeros_like(from_next_side)

    @pl.when(is_first)
    def _():
        from_prev[...] = jnp.zeros_like(from_prev)
        from_prev_side[...] = jnp.zeros_like(from_prev_side)

    @pl.when(jnp.logical_not(is_last))
    def _():
        for direction, copy in rdmas:
            if direction == 0:
                copy.wait_recv()

    @pl.when(jnp.logical_not(is_first))
    def _():
        for direction, copy in rdmas:
            if direction == 1:
                copy.wait_recv()

    side_copy.wait_recv()
    first = sums[1, 0] + from_side[0] + from_prev[0] + from_prev_side[0]
    second = sums[2, 0] + from_side[1] + from_prev[1] + from_prev_side[1] + from_next[...] + from_next_side[...]
    out_ref[0] = first[:, :, :POINTS]
    out_ref[1] = second[:, :, :POINTS]

    for copy in y_copies:
        copy.wait_send()
    for k in range(4):
        wait_sent(k, rows_own, z_send, z_recv)
        wait_sent(k, strip, s_send, s_recv)
    side_copy.wait_send()

    @pl.when(jnp.logical_not(is_first))
    def _():
        for direction, copy in rdmas:
            if direction == 0:
                copy.wait_send()

    @pl.when(jnp.logical_not(is_last))
    def _():
        for direction, copy in rdmas:
            if direction == 1:
                copy.wait_send()


def local_gradient(depth, fixed_image, moving_image, moving_grad):
    high, low = basis_along_x()
    f32 = jnp.float32
    anywhere = pl.BlockSpec(memory_space=pl.ANY)
    dma = pltpu.SemaphoreType.DMA
    return pl.pallas_call(
        functools.partial(kernel, depth),
        out_shape=jax.ShapeDtypeStruct((2, 3, 8, POINTS), f32),
        in_specs=[anywhere] * 5,
        out_specs=pl.BlockSpec(memory_space=pltpu.VMEM),
        scratch_shapes=[
            pltpu.VMEM((5, RAW_PLANES, RAW_ROWS, 128), f32),
            pltpu.VMEM((PLANES, ROWS, 64), f32),
            pltpu.VMEM((PLANES, ROWS, 64), f32),
            pltpu.VMEM((3, 3, PLANES, ROWS, 128), f32),
            pltpu.VMEM((3, PLANES, ROWS, 64), f32),
            pltpu.VMEM((384, 128), jnp.bfloat16),
            pltpu.VMEM((384, 128), jnp.bfloat16),
            pltpu.VMEM((13, COEF_PLANES, RAW_ROWS, 128), f32),
            pltpu.VMEM((2, 13, RAW_ROWS, 128), f32),
            pltpu.VMEM((26, RAW_ROWS, 128), f32),
            pltpu.VMEM((2, 6, 15, 8, 128), f32),
            pltpu.VMEM((2, 6, 15, 8, 128), f32),
            pltpu.VMEM((9, COEF_PLANES, COEF_ROWS, 128), f32),
            pltpu.VMEM((9, PLANES, COEF_ROWS, 128), f32),
            pltpu.VMEM((3, 3, 5, PLANES, 8, 128), f32),
            pltpu.VMEM((240, 384), f32),
            pltpu.VMEM((5, 2, 3, 8, 128), f32),
            pltpu.VMEM((3, 8, 128), f32),
            pltpu.VMEM((2, 3, 8, 128), f32),
            pltpu.VMEM((2, 3, 8, 128), f32),
            pltpu.VMEM((3, 8, 128), f32),
            pltpu.VMEM((2, 3, 8, 128), f32),
            dma((11,)),
            dma((5,)),
            dma((5,)),
            dma((2, 4)),
            dma((2, 4)),
            dma((2, 4)),
            dma((2, 4)),
            dma((5,)),
            dma((5,)),
        ],
        compiler_params=pltpu.CompilerParams(collective_id=0, has_side_effects=True, vmem_limit_bytes=60 * 1024 * 1024),
    )(fixed_image, moving_image, moving_grad, high, low)


def solution(mesh):
    in_specs = (P("gz", "gy", None), P("gz", "gy", None), P(None, "gz", "gy", None))
    out_specs = P("gz", None, "gy", None)
    body = functools.partial(local_gradient, mesh.shape["gz"])
    return jax.shard_map(body, mesh=mesh, in_specs=in_specs, out_specs=out_specs, check_vma=False)
```

```python
import functools

import jax
import jax.numpy as jnp
import numpy as np
from jax import lax
from jax.experimental import pallas as pl
from jax.experimental.pallas import tpu as pltpu
from jax.sharding import PartitionSpec as P

RADIUS = 4
SPACING = 5
EPS = 36.0
SIM_WEIGHT = 8.0
WINDOW = float((2 * RADIUS + 1) ** 3)
MESH = pl.DeviceIdType.MESH

PLANES = 10
ROWS = 40
NX = 320
POINTS = 64
HALO = 2 * RADIUS
RAW_PLANES = PLANES + 2 * HALO
RAW_ROWS = ROWS + 2 * HALO
COEF_PLANES = PLANES + 2 * RADIUS
COEF_ROWS = ROWS + 2 * RADIUS
PAIRS = (0, 8, 2, 6, 4)
UPFRONT = 2


def spline_weights(step):
    u = step / SPACING
    return (
        (1.0 - u) ** 3 / 6.0,
        (3.0 * u**3 - 6.0 * u**2 + 4.0) / 6.0,
        (-3.0 * u**3 + 3.0 * u**2 + 3.0 * u + 1.0) / 6.0,
        u**3 / 6.0,
    )


def basis_along_x():
    matrix = np.zeros((384, 128), np.float64)
    for x in range(NX):
        for k, weight in enumerate(spline_weights(x % SPACING)):
            point = min(max(x // SPACING - 1 + k, 0), POINTS - 1)
            matrix[x, point] += weight
    matrix = matrix.astype(np.float32)
    high = matrix.astype(jnp.bfloat16)
    low = (matrix - high.astype(np.float32)).astype(jnp.bfloat16)
    return high, low


def suffix_sums(values):
    sums = [values[-1]]
    for value in reversed(values[:-1]):
        sums.append(sums[-1] + value)
    return sums[::-1]


def prefix_sums(values):
    sums = [values[0]]
    for value in values[1:]:
        sums.append(sums[-1] + value)
    return sums


def windows_of_nine(values):
    count = len(values) - 8
    if count > 9:
        before = suffix_sums(values[:9])
        after = prefix_sums(values[9:])
        return [before[0]] + [before[i] + after[i - 1] for i in range(1, 9)] + [after[8]]
    common = values[count - 1]
    for value in values[count:9]:
        common = common + value
    before = suffix_sums(values[: count - 1])
    after = prefix_sums(values[9:])
    out = []
    for i in range(count):
        total = common
        if i < count - 1:
            total = total + before[i]
        if i > 0:
            total = total + after[i - 1]
        out.append(total)
    return out


def three_along_x(tiles, reach, lane):
    right = [pltpu.roll(tile, reach, 1) for tile in tiles]
    left = [pltpu.roll(tile, 128 - reach, 1) for tile in tiles]
    out = []
    for i in range(3):
        before = jnp.where(lane < reach, right[i - 1], right[i])
        after = jnp.where(lane >= 128 - reach, left[(i + 1) % 3], left[i])
        out.append(tiles[i] + before + after)
    return out


def kernel(
    depth, f_hbm, m_hbm, g_hbm, bh_hbm, bl_hbm, out_ref,
    raw, f_tail, m_tail, grad, g_tail, bh, bl, own_sum, halo_sum, zsum, stage_y, stage_x, coef, zcoef, weighted, wide,
    sums, passing, from_next, from_prev, from_side, from_next_side, from_prev_side,
    local_sem, y_send, y_recv, z_send, z_recv, s_send, s_recv, hop_send, hop_recv, e_send, e_recv,
):
    gz = lax.axis_index("gz")
    gy = lax.axis_index("gy")
    other = 1 - gy
    is_first = gz == 0
    is_last = gz == depth - 1
    before = (jnp.maximum(gz - 1, 0), gy)
    after = (jnp.minimum(gz + 1, depth - 1), gy)
    before_side = (jnp.maximum(gz - 1, 0), other)
    after_side = (jnp.minimum(gz + 1, depth - 1), other)
    side = (gz, other)
    middle = depth // 2
    detour = depth >= 4
    is_low_mid = (gz == middle - 1) if detour else (gz < 0)
    is_high_mid = (gz == middle) if detour else (gz < 0)

    local = []

    def bring(src, dst):
        copy = pltpu.make_async_copy(src, dst, local_sem.at[len(local)])
        copy.start()
        local.append(copy)

    own = pl.ds(HALO, PLANES)
    rows_own = pl.ds(HALO, ROWS)
    bring(f_hbm.at[:, :, pl.ds(256, 64)], f_tail)
    bring(m_hbm.at[:, :, pl.ds(256, 64)], m_tail)
    for t in range(2):
        bring(f_hbm.at[:, :, pl.ds(128 * t, 128)], raw.at[t, own, rows_own, :])
        bring(m_hbm.at[:, :, pl.ds(128 * t, 128)], raw.at[2 + t, own, rows_own, :])
    for t in range(2):
        bring(g_hbm.at[:, :, :, pl.ds(128 * t, 128)], grad.at[t])
    bring(g_hbm.at[:, :, :, pl.ds(256, 64)], g_tail)
    bring(bh_hbm, bh)
    bring(bl_hbm, bl)

    barrier = pltpu.get_barrier_semaphore()
    pl.semaphore_signal(barrier, inc=1, device_id=side, device_id_type=MESH)

    @pl.when(jnp.logical_not(is_first))
    def _():
        pl.semaphore_signal(barrier, inc=1, device_id=before, device_id_type=MESH)
        pl.semaphore_signal(barrier, inc=1, device_id=before_side, device_id_type=MESH)

    @pl.when(jnp.logical_not(is_last))
    def _():
        pl.semaphore_signal(barrier, inc=1, device_id=after, device_id_type=MESH)
        pl.semaphore_signal(barrier, inc=1, device_id=after_side, device_id_type=MESH)

    if detour:
        @pl.when(is_low_mid | is_high_mid)
        def _():
            for far_slab in (0, depth - 1):
                pl.semaphore_signal(barrier, inc=1, device_id=(far_slab, gy), device_id_type=MESH)

        @pl.when(is_first | is_last)
        def _():
            for far_slab in (middle - 1, middle):
                pl.semaphore_signal(barrier, inc=1, device_id=(far_slab, gy), device_id_type=MESH)

    lane = lax.broadcasted_iota(jnp.int32, (8, 128), 1)
    row = lax.broadcasted_iota(jnp.int32, (8, 128), 0)
    zero = jnp.zeros((8, 128), jnp.float32)
    low_half = lane < 64

    zero_row = pl.multiple_of(48 * gy, 8)
    strip_row = pl.multiple_of(48 - 48 * gy, 8)
    zsum[:, pl.ds(zero_row, 8), :] = jnp.zeros((26, 8, 128), jnp.float32)
    halo_sum[...] = jnp.zeros_like(halo_sum)

    local[0].wait()
    local[1].wait()
    for z in range(PLANES):
        raw[4, HALO + z, HALO : HALO + ROWS, :] = jnp.concatenate([f_tail[z], m_tail[z]], axis=-1)
    for copy in local[2:6]:
        copy.wait()

    if detour:
        @pl.when(is_low_mid | is_high_mid)
        def _():
            pl.semaphore_wait(barrier, 7)

        @pl.when(jnp.logical_not(is_low_mid | is_high_mid))
        def _():
            pl.semaphore_wait(barrier, 5)
    else:
        @pl.when(is_first | is_last)
        def _():
            pl.semaphore_wait(barrier, 3)

        @pl.when(jnp.logical_not(is_first | is_last))
        def _():
            pl.semaphore_wait(barrier, 5)

    src_row = pl.multiple_of(40 - 32 * gy, 8)
    y_copies = []
    for i, first in enumerate(PAIRS):
        copy = pltpu.make_async_remote_copy(
            src_ref=raw.at[:, pl.ds(HALO + first, 2), pl.ds(src_row, 8), :],
            dst_ref=raw.at[:, pl.ds(HALO + first, 2), pl.ds(zero_row, 8), :],
            send_sem=y_send.at[i], recv_sem=y_recv.at[i], device_id=side, device_id_type=MESH,
        )
        copy.start()
        y_copies.append(copy)

    def plane_to_after(k, h):
        return pltpu.make_async_remote_copy(
            src_ref=raw.at[:, 17 - 2 * k - h, rows_own, :],
            dst_ref=raw.at[:, 7 - 2 * k - h, rows_own, :],
            send_sem=z_send.at[0, k, h], recv_sem=z_recv.at[0, k, h], device_id=after, device_id_type=MESH,
        )

    def plane_to_before(k, h):
        return pltpu.make_async_remote_copy(
            src_ref=raw.at[:, 8 + 2 * k + h, rows_own, :],
            dst_ref=raw.at[:, 18 + 2 * k + h, rows_own, :],
            send_sem=z_send.at[1, k, h], recv_sem=z_recv.at[1, k, h], device_id=before, device_id_type=MESH,
        )

    strip = pl.ds(strip_row, 8)

    def strip_to_after(k):
        return pltpu.make_async_remote_copy(
            src_ref=raw.at[:, pl.ds(16 - 2 * k, 2), strip, :],
            dst_ref=raw.at[:, pl.ds(6 - 2 * k, 2), strip, :],
            send_sem=s_send.at[0, k], recv_sem=s_recv.at[0, k], device_id=after, device_id_type=MESH,
        )

    def strip_to_before(k):
        return pltpu.make_async_remote_copy(
            src_ref=raw.at[:, pl.ds(8 + 2 * k, 2), strip, :],
            dst_ref=raw.at[:, pl.ds(18 + 2 * k, 2), strip, :],
            send_sem=s_send.at[1, k], recv_sem=s_recv.at[1, k], device_id=before, device_id_type=MESH,
        )

    def hop_up(k):
        return pltpu.make_async_remote_copy(
            src_ref=raw.at[:, 16 - 2 * k, rows_own, :], dst_ref=passing.at[k],
            send_sem=z_send.at[0, k, 1], recv_sem=hop_recv.at[k], device_id=(depth - 1, gy), device_id_type=MESH,
        )

    def hop_down(k):
        return pltpu.make_async_remote_copy(
            src_ref=raw.at[:, 9 + 2 * k, rows_own, :], dst_ref=passing.at[k],
            send_sem=z_send.at[1, k, 1], recv_sem=hop_recv.at[k], device_id=(0, gy), device_id_type=MESH,
        )

    def on_up(k):
        return pltpu.make_async_remote_copy(
            src_ref=passing.at[k], dst_ref=raw.at[:, 6 - 2 * k, rows_own, :],
            send_sem=hop_send.at[k], recv_sem=z_recv.at[0, k, 1], device_id=(middle, gy), device_id_type=MESH,
        )

    def on_down(k):
        return pltpu.make_async_remote_copy(
            src_ref=passing.at[k], dst_ref=raw.at[:, 19 + 2 * k, rows_own, :],
            send_sem=hop_send.at[k], recv_sem=z_recv.at[1, k, 1], device_id=(middle - 1, gy), device_id_type=MESH,
        )

    sends_up = jnp.logical_not(is_last)
    sends_down = jnp.logical_not(is_first)

    def start_planes(k):
        @pl.when(sends_up)
        def _():
            plane_to_after(k, 0).start()

        @pl.when(sends_down)
        def _():
            plane_to_before(k, 0).start()

        @pl.when(sends_up & jnp.logical_not(is_low_mid))
        def _():
            plane_to_after(k, 1).start()

        @pl.when(sends_down & jnp.logical_not(is_high_mid))
        def _():
            plane_to_before(k, 1).start()

    def start_strips(k):
        @pl.when(sends_up)
        def _():
            strip_to_after(k).start()

        @pl.when(sends_down)
        def _():
            strip_to_before(k).start()

    def pass_on(k):
        if detour:
            @pl.when(is_last)
            def _():
                hop_up(k).wait_recv()
                on_up(k).start()

            @pl.when(is_first)
            def _():
                hop_down(k).wait_recv()
                on_down(k).start()

    def wait_planes(k, h):
        @pl.when(sends_down)
        def _():
            plane_to_after(k, h).wait_recv()

        @pl.when(sends_up)
        def _():
            plane_to_before(k, h).wait_recv()

    def wait_strips(k):
        @pl.when(sends_down)
        def _():
            strip_to_after(k).wait_recv()

        @pl.when(sends_up)
        def _():
            strip_to_before(k).wait_recv()

    if detour:
        @pl.when(is_low_mid)
        def _():
            for k in range(4):
                hop_up(k).start()

        @pl.when(is_high_mid)
        def _():
            for k in range(4):
                hop_down(k).start()

    for k in range(UPFRONT):
        start_planes(k)

    @pl.when(is_first)
    def _():
        raw[:, 0:HALO, :, :] = jnp.zeros((5, HALO, RAW_ROWS, 128), jnp.float32)

    @pl.when(is_last)
    def _():
        raw[:, HALO + PLANES : RAW_PLANES, :, :] = jnp.zeros((5, HALO, RAW_ROWS, 128), jnp.float32)

    def fields_of(plane, rows):
        out = []
        for t in range(2):
            f = raw[t, plane, rows, :]
            m = raw[2 + t, plane, rows, :]
            out += [f, m, f * f, m * m, f * m]
        p = raw[4, plane, rows, :]
        return out + [p, p * p, p * pltpu.roll(p, 64, 1)]

    def own_windows(rows):
        columns = [fields_of(HALO + z, rows) for z in range(PLANES)]
        for col in range(13):
            values = [columns[z][col] for z in range(PLANES)]
            for p, total in enumerate(prefix_sums(values[:9])):
                own_sum[col, p, rows, :] = total
            for p, total in enumerate(suffix_sums(values[1:])):
                own_sum[col, 9 + p, rows, :] = total

    @pl.loop(0, 5)
    def _(i):
        own_windows(pl.ds(pl.multiple_of(8 + 8 * i, 8), 8))

    y_copies[0].wait_recv()
    y_copies[1].wait_recv()
    start_strips(0)
    start_planes(UPFRONT)
    pass_on(0)
    y_copies[2].wait_recv()
    y_copies[3].wait_recv()
    start_strips(1)
    for k in range(UPFRONT + 1, 4):
        start_planes(k)
    y_copies[4].wait_recv()
    start_strips(2)
    start_strips(3)
    for k in range(1, 4):
        pass_on(k)
    own_windows(strip)

    row_valid = []
    for j in range(6):
        position = 6 * row + j + 40 * gy - 4
        row_valid.append(jnp.where((position >= 0) & (position < 80), 1.0, 0.0))

    groups = [pl.ds(8 + 8 * i, 8) for i in range(5)] + [strip]

    def coefficients(planes, halo):
        for s in range(2):
            for rows in groups:
                if halo is None:
                    for col in range(13):
                        zsum[13 * s + col, rows, :] = own_sum[col, planes[s], rows, :]
                else:
                    fields = fields_of(halo[s], rows)
                    for col in range(13):
                        total = halo_sum[s, col, rows, :] + fields[col]
                        halo_sum[s, col, rows, :] = total
                        zsum[13 * s + col, rows, :] = total + own_sum[col, planes[s], rows, :]
        for s in range(2):
            for col in range(13):
                total = windows_of_nine([zsum[13 * s + col, pl.ds(m, 8, stride=6), :] for m in range(14)])
                for j in range(6):
                    if col < 10:
                        stage_y[s, j, 3 * (col % 5) + col // 5] = total[j]
                    elif col == 12:
                        stage_y[s, j, 14] = jnp.where(low_half, total[j], 0.0)
                    else:
                        stage_y[s, j, 6 * (col - 10) + 2] = jnp.where(low_half, total[j], 0.0)
                        stage_y[s, j, 6 * (col - 10) + 5] = jnp.where(low_half, pltpu.roll(total[j], 64, 1), 0.0)
        for s in range(2):
            for j in range(6):
                for i in range(5):
                    three = three_along_x([stage_y[s, j, 3 * i + t] for t in range(3)], 1, lane)
                    for t in range(3):
                        stage_x[s, j, 3 * i + t] = three[t]
        for s in range(2):
            position = gz * PLANES + planes[s] - RADIUS
            inside = jnp.where((position >= 0) & (position < depth * PLANES), 1.0, 0.0)
            for j in range(6):
                boxed = [three_along_x([stage_x[s, j, 3 * i + t] for t in range(3)], 3, lane) for i in range(5)]
                valid = row_valid[j] * inside
                for t in range(3):
                    sf, sm, sff, smm, sfm = [boxed[i][t] for i in range(5)]
                    mf = sf * (1.0 / WINDOW)
                    mm = sm * (1.0 / WINDOW)
                    a = (sfm - mf * sm) * (valid if t < 2 else jnp.where(low_half, valid, 0.0))
                    p = sff - mf * sf + EPS
                    q = smm - mm * sm + EPS
                    r = 1.0 / (p * q)
                    cross = a * r
                    moving = -cross * a * (r * p)
                    where = pl.ds(j, 8, stride=6)
                    coef[t, planes[s], where, :] = cross
                    coef[3 + t, planes[s], where, :] = moving
                    coef[6 + t, planes[s], where, :] = cross * mf + moving * mm

    coefficients((8, 9), None)

    @pl.loop(0, 4)
    def _(k):
        wait_strips(k)

        @pl.loop(0, 2)
        def _(h):
            wait_planes(k, h)
            step = 2 * k + h
            coefficients((7 - step, 10 + step), (7 - step, 18 + step))

    for copy in local[6:]:
        copy.wait()
    grad[2] = jnp.concatenate([g_tail[...], jnp.zeros_like(g_tail)], axis=-1)

    @pl.loop(0, 9)
    def _(col):
        for g in range(6):
            rows = pl.ds(8 * g, 8)
            for z, total in enumerate(windows_of_nine([coef[col, p, rows, :] for p in range(COEF_PLANES)])):
                zcoef[col, z, rows, :] = total

    def slope_planes(planes):
        for s, z in enumerate(planes):
            for col in range(9):
                total = windows_of_nine([zcoef[col, z, pl.ds(m, 8, stride=5), :] for m in range(13)])
                for j in range(5):
                    stage_y[s, j, col] = total[j]
        for s in range(2):
            for j in range(5):
                for i in range(3):
                    three = three_along_x([stage_y[s, j, 3 * i + t] for t in range(3)], 1, lane)
                    for t in range(3):
                        stage_x[s, j, 3 * i + t] = three[t]
        for s, z in enumerate(planes):
            for j in range(5):
                boxed = [three_along_x([stage_x[s, j, 3 * i + t] for t in range(3)], 3, lane) for i in range(3)]
                centre = pl.ds(HALO + j, 8, stride=5)
                tail = raw[4, HALO + z, centre, :]
                f = [raw[0, HALO + z, centre, :], raw[1, HALO + z, centre, :], tail]
                m = [raw[2, HALO + z, centre, :], raw[3, HALO + z, centre, :], pltpu.roll(tail, 64, 1)]
                for t in range(3):
                    slope = f[t] * boxed[0][t] + m[t] * boxed[1][t] - boxed[2][t]
                    for c in range(3):
                        weighted[c, t, j, z] = slope * grad[t, c, z, pl.ds(j, 8, stride=5), :]

    @pl.loop(0, 5)
    def _(z):
        slope_planes((z, z + 5))

    wy = [spline_weights(j) for j in range(SPACING)]
    wz = [[-2.0 * SIM_WEIGHT * w for w in ws] for ws in wy]
    for t in range(3):
        @pl.loop(0, 3)
        def _(c):
            slots = []
            for j in range(SPACING):
                v = [weighted[c, t, j, z] for z in range(PLANES)]
                part = []
                for i in range(2):
                    for k in range(4):
                        total = wz[0][k] * v[5 * i]
                        for step in range(1, SPACING):
                            if wz[step][k] != 0.0:
                                total = total + wz[step][k] * v[5 * i + step]
                        part.append(total)
                slots.append([part[0], part[1] + part[4], part[2] + part[5], part[3] + part[6], part[7]])
            for m in range(5):
                y = []
                for k in range(4):
                    total = wy[0][k] * slots[0][m]
                    for j in range(1, SPACING):
                        total = total + wy[j][k] * slots[j][m]
                    y.append(total)
                r0, r2, r3 = pltpu.roll(y[0], 7, 0), pltpu.roll(y[2], 1, 0), pltpu.roll(y[3], 2, 0)
                inner = (
                    jnp.where(row == 7, 0.0, r0) + y[1] + jnp.where(row == 0, 0.0, r2) + jnp.where(row < 2, 0.0, r3)
                )
                to_low = jnp.where(row == 7, r0, 0.0)
                to_high = jnp.where(row == 0, r2, 0.0) + jnp.where(row < 2, r3, 0.0)
                clip_low = jnp.where(row == 0, y[0], 0.0)
                clip_high = jnp.where(row == 7, y[2] + y[3] + pltpu.roll(y[3], 1, 0), 0.0)
                is_low = gy == 0
                base = pl.multiple_of(48 * m + 8 * c, 8)
                lanes = pl.ds(128 * t, 128)
                wide[pl.ds(base, 8), lanes] = inner + jnp.where(is_low, clip_low, clip_high)
                wide[pl.ds(pl.multiple_of(base + 24, 8), 8), lanes] = jnp.where(is_low, to_high, to_low)

    left = wide[...]
    high = left.astype(jnp.bfloat16)
    low = (left - high.astype(jnp.float32)).astype(jnp.bfloat16)

    def dot(a, b):
        return jnp.dot(a, b, preferred_element_type=jnp.float32)

    total = dot(high, bh[...]) + (dot(low, bh[...]) + dot(high, bl[...]))
    sums[...] = total.reshape(5, 2, 3, 8, 128)

    copies = [
        (0, sums.at[0, 0], from_next, before, 0),
        (0, sums.at[0, 1], from_next_side, before_side, 1),
        (1, sums.at[pl.ds(3, 2), 0], from_prev, after, 2),
        (1, sums.at[pl.ds(3, 2), 1], from_prev_side, after_side, 3),
    ]
    rdmas = [
        (
            direction,
            pltpu.make_async_remote_copy(
                src_ref=src, dst_ref=dst, send_sem=e_send.at[i], recv_sem=e_recv.at[i],
                device_id=target, device_id_type=MESH,
            ),
        )
        for direction, src, dst, target, i in copies
    ]
    side_copy = pltpu.make_async_remote_copy(
        src_ref=sums.at[pl.ds(1, 2), 1], dst_ref=from_side, send_sem=e_send.at[4], recv_sem=e_recv.at[4],
        device_id=side, device_id_type=MESH,
    )

    @pl.when(jnp.logical_not(is_first))
    def _():
        for direction, copy in rdmas:
            if direction == 0:
                copy.start()

    @pl.when(jnp.logical_not(is_last))
    def _():
        for direction, copy in rdmas:
            if direction == 1:
                copy.start()

    low_clip = jnp.where(is_first, 1.0, 0.0)
    high_clip = jnp.where(is_last, 1.0, 0.0)
    sums[1] = sums[1] + low_clip * sums[0]
    sums[2] = sums[2] + high_clip * (sums[3] + sums[4])
    side_copy.start()

    @pl.when(is_last)
    def _():
        from_next[...] = jnp.zeros_like(from_next)
        from_next_side[...] = jnp.zeros_like(from_next_side)

    @pl.when(is_first)
    def _():
        from_prev[...] = jnp.zeros_like(from_prev)
        from_prev_side[...] = jnp.zeros_like(from_prev_side)

    @pl.when(jnp.logical_not(is_last))
    def _():
        for direction, copy in rdmas:
            if direction == 0:
                copy.wait_recv()

    @pl.when(jnp.logical_not(is_first))
    def _():
        for direction, copy in rdmas:
            if direction == 1:
                copy.wait_recv()

    side_copy.wait_recv()
    first = sums[1, 0] + from_side[0] + from_prev[0] + from_prev_side[0]
    second = sums[2, 0] + from_side[1] + from_prev[1] + from_prev_side[1] + from_next[...] + from_next_side[...]
    out_ref[0] = first[:, :, :POINTS]
    out_ref[1] = second[:, :, :POINTS]

    for copy in y_copies:
        copy.wait_send()
    for k in range(4):
        @pl.when(sends_up)
        def _():
            plane_to_after(k, 0).wait_send()
            plane_to_after(k, 1).wait_send()
            strip_to_after(k).wait_send()

        @pl.when(sends_down)
        def _():
            plane_to_before(k, 0).wait_send()
            plane_to_before(k, 1).wait_send()
            strip_to_before(k).wait_send()

        if detour:
            @pl.when(is_first | is_last)
            def _():
                on_up(k).wait_send()
    side_copy.wait_send()

    @pl.when(jnp.logical_not(is_first))
    def _():
        for direction, copy in rdmas:
            if direction == 0:
                copy.wait_send()

    @pl.when(jnp.logical_not(is_last))
    def _():
        for direction, copy in rdmas:
            if direction == 1:
                copy.wait_send()


def local_gradient(depth, fixed_image, moving_image, moving_grad):
    high, low = basis_along_x()
    f32 = jnp.float32
    anywhere = pl.BlockSpec(memory_space=pl.ANY)
    dma = pltpu.SemaphoreType.DMA
    return pl.pallas_call(
        functools.partial(kernel, depth),
        out_shape=jax.ShapeDtypeStruct((2, 3, 8, POINTS), f32),
        in_specs=[anywhere] * 5,
        out_specs=pl.BlockSpec(memory_space=pltpu.VMEM),
        scratch_shapes=[
            pltpu.VMEM((5, RAW_PLANES, RAW_ROWS, 128), f32),
            pltpu.VMEM((PLANES, ROWS, 64), f32),
            pltpu.VMEM((PLANES, ROWS, 64), f32),
            pltpu.VMEM((3, 3, PLANES, ROWS, 128), f32),
            pltpu.VMEM((3, PLANES, ROWS, 64), f32),
            pltpu.VMEM((384, 128), jnp.bfloat16),
            pltpu.VMEM((384, 128), jnp.bfloat16),
            pltpu.VMEM((13, COEF_PLANES, RAW_ROWS, 128), f32),
            pltpu.VMEM((2, 13, RAW_ROWS, 128), f32),
            pltpu.VMEM((26, RAW_ROWS, 128), f32),
            pltpu.VMEM((2, 6, 15, 8, 128), f32),
            pltpu.VMEM((2, 6, 15, 8, 128), f32),
            pltpu.VMEM((9, COEF_PLANES, COEF_ROWS, 128), f32),
            pltpu.VMEM((9, PLANES, COEF_ROWS, 128), f32),
            pltpu.VMEM((3, 3, 5, PLANES, 8, 128), f32),
            pltpu.VMEM((240, 384), f32),
            pltpu.VMEM((5, 2, 3, 8, 128), f32),
            pltpu.VMEM((4, 5, ROWS, 128), f32),
            pltpu.VMEM((3, 8, 128), f32),
            pltpu.VMEM((2, 3, 8, 128), f32),
            pltpu.VMEM((2, 3, 8, 128), f32),
            pltpu.VMEM((3, 8, 128), f32),
            pltpu.VMEM((2, 3, 8, 128), f32),
            dma((11,)),
            dma((5,)),
            dma((5,)),
            dma((2, 4, 2)),
            dma((2, 4, 2)),
            dma((2, 4)),
            dma((2, 4)),
            dma((4,)),
            dma((4,)),
            dma((5,)),
            dma((5,)),
        ],
        compiler_params=pltpu.CompilerParams(collective_id=0, has_side_effects=True, vmem_limit_bytes=60 * 1024 * 1024),
    )(fixed_image, moving_image, moving_grad, high, low)


def solution(mesh):
    in_specs = (P("gz", "gy", None), P("gz", "gy", None), P(None, "gz", "gy", None))
    out_specs = P("gz", None, "gy", None)
    body = functools.partial(local_gradient, mesh.shape["gz"])
    return jax.shard_map(body, mesh=mesh, in_specs=in_specs, out_specs=out_specs, check_vma=False)
```

```python
import functools

import jax
import jax.numpy as jnp
import numpy as np
from jax import lax
from jax.experimental import pallas as pl
from jax.experimental.pallas import tpu as pltpu
from jax.sharding import PartitionSpec as P

RADIUS = 4
SPACING = 5
EPS = 36.0
SIM_WEIGHT = 8.0
WINDOW = float((2 * RADIUS + 1) ** 3)
MESH = pl.DeviceIdType.MESH

PLANES = 10
ROWS = 40
NX = 320
POINTS = 64
HALO = 2 * RADIUS
RAW_PLANES = PLANES + 2 * HALO
RAW_ROWS = ROWS + 2 * HALO
COEF_PLANES = PLANES + 2 * RADIUS
COEF_ROWS = ROWS + 2 * RADIUS
PAIRS = (0, 8, 2, 6, 4)
DETOUR = ((2, 1), (3, 1))


def spline_weights(step):
    u = step / SPACING
    return (
        (1.0 - u) ** 3 / 6.0,
        (3.0 * u**3 - 6.0 * u**2 + 4.0) / 6.0,
        (-3.0 * u**3 + 3.0 * u**2 + 3.0 * u + 1.0) / 6.0,
        u**3 / 6.0,
    )


def basis_along_x():
    matrix = np.zeros((384, 128), np.float64)
    for x in range(NX):
        for k, weight in enumerate(spline_weights(x % SPACING)):
            point = min(max(x // SPACING - 1 + k, 0), POINTS - 1)
            matrix[x, point] += weight
    matrix = matrix.astype(np.float32)
    high = matrix.astype(jnp.bfloat16)
    low = (matrix - high.astype(np.float32)).astype(jnp.bfloat16)
    return high, low


def suffix_sums(values):
    sums = [values[-1]]
    for value in reversed(values[:-1]):
        sums.append(sums[-1] + value)
    return sums[::-1]


def prefix_sums(values):
    sums = [values[0]]
    for value in values[1:]:
        sums.append(sums[-1] + value)
    return sums


def windows_of_nine(values):
    count = len(values) - 8
    if count > 9:
        before = suffix_sums(values[:9])
        after = prefix_sums(values[9:])
        return [before[0]] + [before[i] + after[i - 1] for i in range(1, 9)] + [after[8]]
    common = values[count - 1]
    for value in values[count:9]:
        common = common + value
    before = suffix_sums(values[: count - 1])
    after = prefix_sums(values[9:])
    out = []
    for i in range(count):
        total = common
        if i < count - 1:
            total = total + before[i]
        if i > 0:
            total = total + after[i - 1]
        out.append(total)
    return out


def three_along_x(tiles, reach, lane):
    right = [pltpu.roll(tile, reach, 1) for tile in tiles]
    left = [pltpu.roll(tile, 128 - reach, 1) for tile in tiles]
    out = []
    for i in range(3):
        before = jnp.where(lane < reach, right[i - 1], right[i])
        after = jnp.where(lane >= 128 - reach, left[(i + 1) % 3], left[i])
        out.append(tiles[i] + before + after)
    return out


def kernel(
    depth, f_hbm, m_hbm, g_hbm, bh_hbm, bl_hbm, out_ref,
    raw, f_tail, m_tail, grad, g_tail, bh, bl, own_sum, halo_sum, zsum, ysum, stage_y, stage_x, coef, weighted, inner_sum, wide,
    sums, passing, from_next, from_prev, from_side, from_next_side, from_prev_side,
    local_sem, y_send, y_recv, z_send, z_recv, s_send, s_recv, hop_send, hop_recv, e_send, e_recv,
):
    gz = lax.axis_index("gz")
    gy = lax.axis_index("gy")
    other = 1 - gy
    is_first = gz == 0
    is_last = gz == depth - 1
    before = (jnp.maximum(gz - 1, 0), gy)
    after = (jnp.minimum(gz + 1, depth - 1), gy)
    before_side = (jnp.maximum(gz - 1, 0), other)
    after_side = (jnp.minimum(gz + 1, depth - 1), other)
    side = (gz, other)
    middle = depth // 2
    detour = depth >= 4 and len(DETOUR) > 0
    is_low_mid = (gz == middle - 1) if detour else (gz < 0)
    is_high_mid = (gz == middle) if detour else (gz < 0)

    local = []

    def bring(src, dst):
        copy = pltpu.make_async_copy(src, dst, local_sem.at[len(local)])
        copy.start()
        local.append(copy)

    own = pl.ds(HALO, PLANES)
    rows_own = pl.ds(HALO, ROWS)
    bring(f_hbm.at[:, :, pl.ds(256, 64)], f_tail)
    bring(m_hbm.at[:, :, pl.ds(256, 64)], m_tail)
    for t in range(2):
        bring(f_hbm.at[:, :, pl.ds(128 * t, 128)], raw.at[t, own, rows_own, :])
        bring(m_hbm.at[:, :, pl.ds(128 * t, 128)], raw.at[2 + t, own, rows_own, :])
    for t in range(2):
        bring(g_hbm.at[:, :, :, pl.ds(128 * t, 128)], grad.at[t])
    bring(g_hbm.at[:, :, :, pl.ds(256, 64)], g_tail)
    bring(bh_hbm, bh)
    bring(bl_hbm, bl)

    barrier = pltpu.get_barrier_semaphore()
    pl.semaphore_signal(barrier, inc=1, device_id=side, device_id_type=MESH)

    @pl.when(jnp.logical_not(is_first))
    def _():
        pl.semaphore_signal(barrier, inc=1, device_id=before, device_id_type=MESH)
        pl.semaphore_signal(barrier, inc=1, device_id=before_side, device_id_type=MESH)

    @pl.when(jnp.logical_not(is_last))
    def _():
        pl.semaphore_signal(barrier, inc=1, device_id=after, device_id_type=MESH)
        pl.semaphore_signal(barrier, inc=1, device_id=after_side, device_id_type=MESH)

    if detour:
        @pl.when(is_low_mid | is_high_mid)
        def _():
            for far_slab in (0, depth - 1):
                pl.semaphore_signal(barrier, inc=1, device_id=(far_slab, gy), device_id_type=MESH)

        @pl.when(is_first | is_last)
        def _():
            for far_slab in (middle - 1, middle):
                pl.semaphore_signal(barrier, inc=1, device_id=(far_slab, gy), device_id_type=MESH)

    lane = lax.broadcasted_iota(jnp.int32, (8, 128), 1)
    row = lax.broadcasted_iota(jnp.int32, (8, 128), 0)
    zero = jnp.zeros((8, 128), jnp.float32)
    low_half = lane < 64

    zero_row = pl.multiple_of(48 * gy, 8)
    strip_row = pl.multiple_of(48 - 48 * gy, 8)
    raw[:, :, pl.ds(zero_row, 8), :] = jnp.zeros((5, RAW_PLANES, 8, 128), jnp.float32)
    halo_sum[...] = jnp.zeros_like(halo_sum)
    main_row = pl.multiple_of(8 * gy, 8)
    edge_row = pl.multiple_of(40 - 40 * gy, 8)

    local[0].wait()
    local[1].wait()
    for z in range(PLANES):
        raw[4, HALO + z, HALO : HALO + ROWS, :] = jnp.concatenate([f_tail[z], m_tail[z]], axis=-1)
    for copy in local[2:6]:
        copy.wait()

    if detour:
        @pl.when(is_low_mid | is_high_mid)
        def _():
            pl.semaphore_wait(barrier, 7)

        @pl.when(jnp.logical_not(is_low_mid | is_high_mid))
        def _():
            pl.semaphore_wait(barrier, 5)
    else:
        @pl.when(is_first | is_last)
        def _():
            pl.semaphore_wait(barrier, 3)

        @pl.when(jnp.logical_not(is_first | is_last))
        def _():
            pl.semaphore_wait(barrier, 5)

    src_row = pl.multiple_of(40 - 32 * gy, 8)
    y_copies = []
    for i, first in enumerate(PAIRS):
        copy = pltpu.make_async_remote_copy(
            src_ref=raw.at[:, pl.ds(HALO + first, 2), pl.ds(src_row, 8), :],
            dst_ref=raw.at[:, pl.ds(HALO + first, 2), pl.ds(zero_row, 8), :],
            send_sem=y_send.at[i], recv_sem=y_recv.at[i], device_id=side, device_id_type=MESH,
        )
        copy.start()
        y_copies.append(copy)

    def plane_to_after(k, h):
        return pltpu.make_async_remote_copy(
            src_ref=raw.at[:, 17 - 2 * k - h, rows_own, :],
            dst_ref=raw.at[:, 7 - 2 * k - h, rows_own, :],
            send_sem=z_send.at[0, k, h], recv_sem=z_recv.at[0, k, h], device_id=after, device_id_type=MESH,
        )

    def plane_to_before(k, h):
        return pltpu.make_async_remote_copy(
            src_ref=raw.at[:, 8 + 2 * k + h, rows_own, :],
            dst_ref=raw.at[:, 18 + 2 * k + h, rows_own, :],
            send_sem=z_send.at[1, k, h], recv_sem=z_recv.at[1, k, h], device_id=before, device_id_type=MESH,
        )

    strip = pl.ds(strip_row, 8)

    def strip_to_after(k):
        return pltpu.make_async_remote_copy(
            src_ref=raw.at[:, pl.ds(16 - 2 * k, 2), strip, :],
            dst_ref=raw.at[:, pl.ds(6 - 2 * k, 2), strip, :],
            send_sem=s_send.at[0, k], recv_sem=s_recv.at[0, k], device_id=after, device_id_type=MESH,
        )

    def strip_to_before(k):
        return pltpu.make_async_remote_copy(
            src_ref=raw.at[:, pl.ds(8 + 2 * k, 2), strip, :],
            dst_ref=raw.at[:, pl.ds(18 + 2 * k, 2), strip, :],
            send_sem=s_send.at[1, k], recv_sem=s_recv.at[1, k], device_id=before, device_id_type=MESH,
        )

    def hop_up(i):
        k, h = DETOUR[i]
        return pltpu.make_async_remote_copy(
            src_ref=raw.at[:, 17 - 2 * k - h, rows_own, :], dst_ref=passing.at[i],
            send_sem=z_send.at[0, k, h], recv_sem=hop_recv.at[i], device_id=(depth - 1, gy), device_id_type=MESH,
        )

    def hop_down(i):
        k, h = DETOUR[i]
        return pltpu.make_async_remote_copy(
            src_ref=raw.at[:, 8 + 2 * k + h, rows_own, :], dst_ref=passing.at[i],
            send_sem=z_send.at[1, k, h], recv_sem=hop_recv.at[i], device_id=(0, gy), device_id_type=MESH,
        )

    def on_up(i):
        k, h = DETOUR[i]
        return pltpu.make_async_remote_copy(
            src_ref=passing.at[i], dst_ref=raw.at[:, 7 - 2 * k - h, rows_own, :],
            send_sem=hop_send.at[i], recv_sem=z_recv.at[0, k, h], device_id=(middle, gy), device_id_type=MESH,
        )

    def on_down(i):
        k, h = DETOUR[i]
        return pltpu.make_async_remote_copy(
            src_ref=passing.at[i], dst_ref=raw.at[:, 18 + 2 * k + h, rows_own, :],
            send_sem=hop_send.at[i], recv_sem=z_recv.at[1, k, h], device_id=(middle - 1, gy), device_id_type=MESH,
        )

    sends_up = jnp.logical_not(is_last)
    sends_down = jnp.logical_not(is_first)

    def start_plane(k, h):
        goes_round = (k, h) in DETOUR
        up = sends_up & jnp.logical_not(is_low_mid) if goes_round else sends_up
        down = sends_down & jnp.logical_not(is_high_mid) if goes_round else sends_down

        @pl.when(up)
        def _():
            plane_to_after(k, h).start()

        @pl.when(down)
        def _():
            plane_to_before(k, h).start()

    def start_strips(k):
        @pl.when(sends_up)
        def _():
            strip_to_after(k).start()

        @pl.when(sends_down)
        def _():
            strip_to_before(k).start()

    def pass_on(i):
        if detour and i < len(DETOUR):
            @pl.when(is_last)
            def _():
                hop_up(i).wait_recv()
                on_up(i).start()

            @pl.when(is_first)
            def _():
                hop_down(i).wait_recv()
                on_down(i).start()

    def wait_planes(k, h):
        @pl.when(sends_down)
        def _():
            plane_to_after(k, h).wait_recv()

        @pl.when(sends_up)
        def _():
            plane_to_before(k, h).wait_recv()

    def wait_strips(k):
        @pl.when(sends_down)
        def _():
            strip_to_after(k).wait_recv()

        @pl.when(sends_up)
        def _():
            strip_to_before(k).wait_recv()

    if detour:
        @pl.when(is_low_mid)
        def _():
            for i in range(len(DETOUR)):
                hop_up(i).start()

        @pl.when(is_high_mid)
        def _():
            for i in range(len(DETOUR)):
                hop_down(i).start()

    for k, h in ((0, 0), (0, 1), (1, 0), (1, 1), (2, 0)):
        start_plane(k, h)

    @pl.when(is_first)
    def _():
        raw[:, 0:HALO, :, :] = jnp.zeros((5, HALO, RAW_ROWS, 128), jnp.float32)

    @pl.when(is_last)
    def _():
        raw[:, HALO + PLANES : RAW_PLANES, :, :] = jnp.zeros((5, HALO, RAW_ROWS, 128), jnp.float32)

    def fields_of(plane, rows):
        out = []
        for t in range(2):
            f = raw[t, plane, rows, :]
            m = raw[2 + t, plane, rows, :]
            out += [f, m, f * f, m * m, f * m]
        p = raw[4, plane, rows, :]
        return out + [p, p * p, p * pltpu.roll(p, 64, 1)]

    def own_windows(rows):
        columns = [fields_of(HALO + z, rows) for z in range(PLANES)]
        for col in range(13):
            values = [columns[z][col] for z in range(PLANES)]
            for p, total in enumerate(prefix_sums(values[:9])):
                own_sum[col, p, rows, :] = total
            for p, total in enumerate(suffix_sums(values[1:])):
                own_sum[col, 9 + p, rows, :] = total

    @pl.loop(0, 6)
    def _(i):
        own_windows(pl.ds(pl.multiple_of(main_row + 8 * i, 8), 8))

    def coefficients(items, base, count, part):
        offset = 48 * part
        for n, (plane, halo, side_of) in enumerate(items):
            for g in range(count + 1):
                rows = pl.ds(pl.multiple_of(base + 8 * g, 8), 8)
                here = pl.ds(8 * g, 8)
                if halo is None:
                    for col in range(13):
                        zsum[13 * n + col, here, :] = own_sum[col, plane, rows, :]
                else:
                    there = pl.ds(offset + 8 * g, 8)
                    fields = fields_of(halo, rows)
                    for col in range(13):
                        total = halo_sum[side_of, col, there, :] + fields[col]
                        halo_sum[side_of, col, there, :] = total
                        zsum[13 * n + col, here, :] = total + own_sum[col, plane, rows, :]
        for n in range(len(items)):
            for col in range(13):
                at = 13 * n + col
                for g in range(count + 1):
                    ysum[at, pl.ds(8 * g, 8), :] = (
                        zsum[at, pl.ds(8 * g, 8), :] + zsum[at, pl.ds(8 * g + 1, 8), :] + zsum[at, pl.ds(8 * g + 2, 8), :]
                    )
                for j in range(count):
                    total = (
                        ysum[at, pl.ds(8 * j, 8), :] + ysum[at, pl.ds(8 * j + 3, 8), :] + ysum[at, pl.ds(8 * j + 6, 8), :]
                    )
                    if col < 10:
                        stage_y[n, j, 3 * (col % 5) + col // 5] = total
                    elif col == 12:
                        stage_y[n, j, 14] = jnp.where(low_half, total, 0.0)
                    else:
                        stage_y[n, j, 6 * (col - 10) + 2] = jnp.where(low_half, total, 0.0)
                        stage_y[n, j, 6 * (col - 10) + 5] = jnp.where(low_half, pltpu.roll(total, 64, 1), 0.0)
        for n in range(len(items)):
            for j in range(count):
                for i in range(5):
                    three = three_along_x([stage_y[n, j, 3 * i + t] for t in range(3)], 1, lane)
                    for t in range(3):
                        stage_x[n, j, 3 * i + t] = three[t]
        for n, (plane, halo, side_of) in enumerate(items):
            position = gz * PLANES + plane - RADIUS
            inside = (position >= 0) & (position < depth * PLANES)
            for j in range(count):
                boxed = [three_along_x([stage_x[n, j, 3 * i + t] for t in range(3)], 3, lane) for i in range(5)]
                position = base + 8 * j + row + 40 * gy - RADIUS
                valid = jnp.where(inside & (position >= 0) & (position < 80), 1.0, 0.0)
                where = pl.ds(pl.multiple_of(base + 8 * j, 8), 8)
                for t in range(3):
                    sf, sm, sff, smm, sfm = [boxed[i][t] for i in range(5)]
                    mf = sf * (1.0 / WINDOW)
                    mm = sm * (1.0 / WINDOW)
                    a = (sfm - mf * sm) * (valid if t < 2 else jnp.where(low_half, valid, 0.0))
                    p = sff - mf * sf + EPS
                    q = smm - mm * sm + EPS
                    r = 1.0 / (p * q)
                    cross = a * r
                    moving = -cross * a * (r * p)
                    for i, value in enumerate((cross, moving, cross * mf + moving * mm)):
                        if halo is not None:
                            value = value + coef[3 * i + t, plane + (1, -1)[side_of], where, :]
                        coef[3 * i + t, plane, where, :] = value

    middle_items = [(8, None, 0), (9, None, 1)]

    def step_items(step):
        return [(7 - step, 7 - step, 0), (10 + step, 18 + step, 1)]

    def main_part(items):
        coefficients(items, main_row, 5, 0)

    def edge_part(items):
        coefficients(items, edge_row, 1, 1)

    def slope_planes(planes, ends):
        for s, z in enumerate(planes):
            for col in range(9):
                values = []
                for m in range(13):
                    where = pl.ds(m, 8, stride=5)
                    if ends:
                        values.append(coef[col, (0, COEF_PLANES - 1)[s], where, :])
                    else:
                        values.append(coef[col, z, where, :] + coef[col, z + 2 * RADIUS, where, :])
                total = windows_of_nine(values)
                for j in range(5):
                    stage_y[s, j, col] = total[j]
        for s in range(2):
            for j in range(5):
                for i in range(3):
                    three = three_along_x([stage_y[s, j, 3 * i + t] for t in range(3)], 1, lane)
                    for t in range(3):
                        stage_x[s, j, 3 * i + t] = three[t]
        for s, z in enumerate(planes):
            for j in range(5):
                boxed = [three_along_x([stage_x[s, j, 3 * i + t] for t in range(3)], 3, lane) for i in range(3)]
                centre = pl.ds(HALO + j, 8, stride=5)
                tail = raw[4, HALO + z, centre, :]
                f = [raw[0, HALO + z, centre, :], raw[1, HALO + z, centre, :], tail]
                m = [raw[2, HALO + z, centre, :], raw[3, HALO + z, centre, :], pltpu.roll(tail, 64, 1)]
                for t in range(3):
                    slope = f[t] * boxed[0][t] + m[t] * boxed[1][t] - boxed[2][t]
                    for c in range(3):
                        weighted[c, t, j, z] = slope * grad[t, c, z, pl.ds(j, 8, stride=5), :]

    main_part(middle_items)

    for copy in local[6:]:
        copy.wait()
    grad[2] = jnp.concatenate([g_tail[...], jnp.zeros_like(g_tail)], axis=-1)

    @pl.loop(0, 7)
    def _(step):
        wait_planes(step // 2, step % 2)
        main_part(step_items(step))

        @pl.when(step == 0)
        def _():
            pass_on(0)

        @pl.when(step == 1)
        def _():
            y_copies[0].wait_recv()
            y_copies[1].wait_recv()
            start_strips(0)
            start_plane(2, 1)
            start_plane(3, 0)
            pass_on(1)

        @pl.when(step == 2)
        def _():
            y_copies[2].wait_recv()
            y_copies[3].wait_recv()
            start_strips(1)
            pass_on(2)

        @pl.when(step == 3)
        def _():
            y_copies[4].wait_recv()
            start_strips(2)
            start_strips(3)
            start_plane(3, 1)
            pass_on(3)
            own_windows(strip)

        @pl.when(step == 5)
        def _():
            wait_strips(0)
            wait_strips(1)
            edge_part(middle_items + step_items(0) + step_items(1) + step_items(2))

    wait_strips(2)
    wait_strips(3)
    edge_part(step_items(3) + step_items(4) + step_items(5) + step_items(6))

    @pl.loop(3, 7)
    def _(step):
        slope_planes((7 - step, 2 + step), False)

    wy = [spline_weights(j) for j in range(SPACING)]
    wz = [[-2.0 * SIM_WEIGHT * w for w in ws] for ws in wy]

    def add_plane(slots, z, value):
        for k in range(4):
            weight = wz[z % SPACING][k]
            if weight != 0.0:
                m = z // SPACING + k
                slots[m] = weight * value if slots[m] is None else slots[m] + weight * value

    for t in range(3):
        @pl.loop(0, 3)
        def _(c):
            for j in range(SPACING):
                slots = [None] * 5
                for z in range(1, PLANES - 1):
                    add_plane(slots, z, weighted[c, t, j, z])
                for m in range(5):
                    inner_sum[c, t, j, m] = slots[m]

    wait_planes(3, 1)
    main_part(step_items(7))
    edge_part(step_items(7))
    slope_planes((0, PLANES - 1), True)

    for t in range(3):
        @pl.loop(0, 3)
        def _(c):
            slots = []
            for j in range(SPACING):
                parts = [inner_sum[c, t, j, m] for m in range(5)]
                add_plane(parts, 0, weighted[c, t, j, 0])
                add_plane(parts, PLANES - 1, weighted[c, t, j, PLANES - 1])
                slots.append(parts)
            for m in range(5):
                y = []
                for k in range(4):
                    total = wy[0][k] * slots[0][m]
                    for j in range(1, SPACING):
                        total = total + wy[j][k] * slots[j][m]
                    y.append(total)
                r0, r2, r3 = pltpu.roll(y[0], 7, 0), pltpu.roll(y[2], 1, 0), pltpu.roll(y[3], 2, 0)
                inner = (
                    jnp.where(row == 7, 0.0, r0) + y[1] + jnp.where(row == 0, 0.0, r2) + jnp.where(row < 2, 0.0, r3)
                )
                to_low = jnp.where(row == 7, r0, 0.0)
                to_high = jnp.where(row == 0, r2, 0.0) + jnp.where(row < 2, r3, 0.0)
                clip_low = jnp.where(row == 0, y[0], 0.0)
                clip_high = jnp.where(row == 7, y[2] + y[3] + pltpu.roll(y[3], 1, 0), 0.0)
                is_low = gy == 0
                base = pl.multiple_of(48 * m + 8 * c, 8)
                lanes = pl.ds(128 * t, 128)
                wide[pl.ds(base, 8), lanes] = inner + jnp.where(is_low, clip_low, clip_high)
                wide[pl.ds(pl.multiple_of(base + 24, 8), 8), lanes] = jnp.where(is_low, to_high, to_low)

    left = wide[...]
    high = left.astype(jnp.bfloat16)
    low = (left - high.astype(jnp.float32)).astype(jnp.bfloat16)

    def dot(a, b):
        return jnp.dot(a, b, preferred_element_type=jnp.float32)

    total = dot(high, bh[...]) + (dot(low, bh[...]) + dot(high, bl[...]))
    sums[...] = total.reshape(5, 2, 3, 8, 128)

    copies = [
        (0, sums.at[0, 0], from_next, before, 0),
        (0, sums.at[0, 1], from_next_side, before_side, 1),
        (1, sums.at[pl.ds(3, 2), 0], from_prev, after, 2),
        (1, sums.at[pl.ds(3, 2), 1], from_prev_side, after_side, 3),
    ]
    rdmas = [
        (
            direction,
            pltpu.make_async_remote_copy(
                src_ref=src, dst_ref=dst, send_sem=e_send.at[i], recv_sem=e_recv.at[i],
                device_id=target, device_id_type=MESH,
            ),
        )
        for direction, src, dst, target, i in copies
    ]
    side_copy = pltpu.make_async_remote_copy(
        src_ref=sums.at[pl.ds(1, 2), 1], dst_ref=from_side, send_sem=e_send.at[4], recv_sem=e_recv.at[4],
        device_id=side, device_id_type=MESH,
    )

    @pl.when(jnp.logical_not(is_first))
    def _():
        for direction, copy in rdmas:
            if direction == 0:
                copy.start()

    @pl.when(jnp.logical_not(is_last))
    def _():
        for direction, copy in rdmas:
            if direction == 1:
                copy.start()

    low_clip = jnp.where(is_first, 1.0, 0.0)
    high_clip = jnp.where(is_last, 1.0, 0.0)
    sums[1] = sums[1] + low_clip * sums[0]
    sums[2] = sums[2] + high_clip * (sums[3] + sums[4])
    side_copy.start()

    @pl.when(is_last)
    def _():
        from_next[...] = jnp.zeros_like(from_next)
        from_next_side[...] = jnp.zeros_like(from_next_side)

    @pl.when(is_first)
    def _():
        from_prev[...] = jnp.zeros_like(from_prev)
        from_prev_side[...] = jnp.zeros_like(from_prev_side)

    @pl.when(jnp.logical_not(is_last))
    def _():
        for direction, copy in rdmas:
            if direction == 0:
                copy.wait_recv()

    @pl.when(jnp.logical_not(is_first))
    def _():
        for direction, copy in rdmas:
            if direction == 1:
                copy.wait_recv()

    side_copy.wait_recv()
    first = sums[1, 0] + from_side[0] + from_prev[0] + from_prev_side[0]
    second = sums[2, 0] + from_side[1] + from_prev[1] + from_prev_side[1] + from_next[...] + from_next_side[...]
    out_ref[0] = first[:, :, :POINTS]
    out_ref[1] = second[:, :, :POINTS]

    for copy in y_copies:
        copy.wait_send()
    for k in range(4):
        @pl.when(sends_up)
        def _():
            plane_to_after(k, 0).wait_send()
            plane_to_after(k, 1).wait_send()
            strip_to_after(k).wait_send()

        @pl.when(sends_down)
        def _():
            plane_to_before(k, 0).wait_send()
            plane_to_before(k, 1).wait_send()
            strip_to_before(k).wait_send()

        if detour and k < len(DETOUR):
            @pl.when(is_first | is_last)
            def _():
                on_up(k).wait_send()
    side_copy.wait_send()

    @pl.when(jnp.logical_not(is_first))
    def _():
        for direction, copy in rdmas:
            if direction == 0:
                copy.wait_send()

    @pl.when(jnp.logical_not(is_last))
    def _():
        for direction, copy in rdmas:
            if direction == 1:
                copy.wait_send()


def local_gradient(depth, fixed_image, moving_image, moving_grad):
    high, low = basis_along_x()
    f32 = jnp.float32
    anywhere = pl.BlockSpec(memory_space=pl.ANY)
    dma = pltpu.SemaphoreType.DMA
    return pl.pallas_call(
        functools.partial(kernel, depth),
        out_shape=jax.ShapeDtypeStruct((2, 3, 8, POINTS), f32),
        in_specs=[anywhere] * 5,
        out_specs=pl.BlockSpec(memory_space=pltpu.VMEM),
        scratch_shapes=[
            pltpu.VMEM((5, RAW_PLANES, RAW_ROWS, 128), f32),
            pltpu.VMEM((PLANES, ROWS, 64), f32),
            pltpu.VMEM((PLANES, ROWS, 64), f32),
            pltpu.VMEM((3, 3, PLANES, ROWS, 128), f32),
            pltpu.VMEM((3, PLANES, ROWS, 64), f32),
            pltpu.VMEM((384, 128), jnp.bfloat16),
            pltpu.VMEM((384, 128), jnp.bfloat16),
            pltpu.VMEM((13, COEF_PLANES, RAW_ROWS, 128), f32),
            pltpu.VMEM((2, 13, 64, 128), f32),
            pltpu.VMEM((104, RAW_ROWS, 128), f32),
            pltpu.VMEM((104, RAW_ROWS, 128), f32),
            pltpu.VMEM((8, 5, 15, 8, 128), f32),
            pltpu.VMEM((8, 5, 15, 8, 128), f32),
            pltpu.VMEM((9, COEF_PLANES, COEF_ROWS, 128), f32),
            pltpu.VMEM((3, 3, 5, PLANES, 8, 128), f32),
            pltpu.VMEM((3, 3, 5, 5, 8, 128), f32),
            pltpu.VMEM((240, 384), f32),
            pltpu.VMEM((5, 2, 3, 8, 128), f32),
            pltpu.VMEM((4, 5, ROWS, 128), f32),
            pltpu.VMEM((3, 8, 128), f32),
            pltpu.VMEM((2, 3, 8, 128), f32),
            pltpu.VMEM((2, 3, 8, 128), f32),
            pltpu.VMEM((3, 8, 128), f32),
            pltpu.VMEM((2, 3, 8, 128), f32),
            dma((11,)),
            dma((5,)),
            dma((5,)),
            dma((2, 4, 2)),
            dma((2, 4, 2)),
            dma((2, 4)),
            dma((2, 4)),
            dma((4,)),
            dma((4,)),
            dma((5,)),
            dma((5,)),
        ],
        compiler_params=pltpu.CompilerParams(collective_id=0, has_side_effects=True, vmem_limit_bytes=56500000),
    )(fixed_image, moving_image, moving_grad, high, low)


def solution(mesh):
    in_specs = (P("gz", "gy", None), P("gz", "gy", None), P(None, "gz", "gy", None))
    out_specs = P("gz", None, "gy", None)
    body = functools.partial(local_gradient, mesh.shape["gz"])
    return jax.shard_map(body, mesh=mesh, in_specs=in_specs, out_specs=out_specs, check_vma=False)
```

```python
import functools

import jax
import jax.numpy as jnp
import numpy as np
from jax import lax
from jax.experimental import pallas as pl
from jax.experimental.pallas import tpu as pltpu
from jax.sharding import PartitionSpec as P

RADIUS = 4
SPACING = 5
EPS = 36.0
SIM_WEIGHT = 8.0
WINDOW = float((2 * RADIUS + 1) ** 3)
MESH = pl.DeviceIdType.MESH

PLANES = 10
ROWS = 40
NX = 320
POINTS = 64
HALO = 2 * RADIUS
RAW_PLANES = PLANES + 2 * HALO
RAW_ROWS = ROWS + 2 * HALO
COEF_PLANES = PLANES + 2 * RADIUS
COEF_ROWS = ROWS + 2 * RADIUS
PAIRS = (0, 8, 2, 6, 4)
DETOUR = (((2, 0), 0), ((2, 1), 0), ((3, 0), 0), ((3, 1), 0))
PASS_AFTER = (3, 4, 5, 6)
ROUND = tuple(plane for plane, way in DETOUR)


def spline_weights(step):
    u = step / SPACING
    return (
        (1.0 - u) ** 3 / 6.0,
        (3.0 * u**3 - 6.0 * u**2 + 4.0) / 6.0,
        (-3.0 * u**3 + 3.0 * u**2 + 3.0 * u + 1.0) / 6.0,
        u**3 / 6.0,
    )


def basis_along_x():
    matrix = np.zeros((384, 128), np.float64)
    for x in range(NX):
        for k, weight in enumerate(spline_weights(x % SPACING)):
            point = min(max(x // SPACING - 1 + k, 0), POINTS - 1)
            matrix[x, point] += weight
    matrix = matrix.astype(np.float32)
    high = matrix.astype(jnp.bfloat16)
    low = (matrix - high.astype(np.float32)).astype(jnp.bfloat16)
    return high, low


def suffix_sums(values):
    sums = [values[-1]]
    for value in reversed(values[:-1]):
        sums.append(sums[-1] + value)
    return sums[::-1]


def prefix_sums(values):
    sums = [values[0]]
    for value in values[1:]:
        sums.append(sums[-1] + value)
    return sums


def windows_of_nine(values):
    count = len(values) - 8
    if count > 9:
        before = suffix_sums(values[:9])
        after = prefix_sums(values[9:])
        return [before[0]] + [before[i] + after[i - 1] for i in range(1, 9)] + [after[8]]
    common = values[count - 1]
    for value in values[count:9]:
        common = common + value
    before = suffix_sums(values[: count - 1])
    after = prefix_sums(values[9:])
    out = []
    for i in range(count):
        total = common
        if i < count - 1:
            total = total + before[i]
        if i > 0:
            total = total + after[i - 1]
        out.append(total)
    return out


def three_along_x(tiles, reach, lane):
    right = [pltpu.roll(tile, reach, 1) for tile in tiles]
    left = [pltpu.roll(tile, 128 - reach, 1) for tile in tiles]
    out = []
    for i in range(3):
        before = jnp.where(lane < reach, right[i - 1], right[i])
        after = jnp.where(lane >= 128 - reach, left[(i + 1) % 3], left[i])
        out.append(tiles[i] + before + after)
    return out


def kernel(
    depth, f_hbm, m_hbm, g_hbm, bh_hbm, bl_hbm, out_ref,
    raw, f_tail, m_tail, grad, g_tail, bh, bl, own_sum, halo_sum, zsum, ysum, stage_y, stage_x, coef, weighted, inner_sum, wide,
    sums, passing, from_next, from_prev, from_side, from_next_side, from_prev_side,
    local_sem, y_send, y_recv, z_send, z_recv, s_send, s_recv, hop_send, hop_recv, e_send, e_recv,
):
    gz = lax.axis_index("gz")
    gy = lax.axis_index("gy")
    other = 1 - gy
    is_first = gz == 0
    is_last = gz == depth - 1
    before = (jnp.maximum(gz - 1, 0), gy)
    after = (jnp.minimum(gz + 1, depth - 1), gy)
    before_side = (jnp.maximum(gz - 1, 0), other)
    after_side = (jnp.minimum(gz + 1, depth - 1), other)
    side = (gz, other)
    middle = depth // 2
    detour = depth >= 4 and len(DETOUR) > 0
    is_low_mid = (gz == middle - 1) if detour else (gz < 0)
    is_high_mid = (gz == middle) if detour else (gz < 0)

    local = []

    def bring(src, dst):
        copy = pltpu.make_async_copy(src, dst, local_sem.at[len(local)])
        copy.start()
        local.append(copy)

    own = pl.ds(HALO, PLANES)
    rows_own = pl.ds(HALO, ROWS)
    bring(f_hbm.at[:, :, pl.ds(256, 64)], f_tail)
    bring(m_hbm.at[:, :, pl.ds(256, 64)], m_tail)
    for t in range(2):
        bring(f_hbm.at[:, :, pl.ds(128 * t, 128)], raw.at[t, own, rows_own, :])
        bring(m_hbm.at[:, :, pl.ds(128 * t, 128)], raw.at[2 + t, own, rows_own, :])
    for t in range(2):
        bring(g_hbm.at[:, :, :, pl.ds(128 * t, 128)], grad.at[t])
    bring(g_hbm.at[:, :, :, pl.ds(256, 64)], g_tail)
    bring(bh_hbm, bh)
    bring(bl_hbm, bl)

    barrier = pltpu.get_barrier_semaphore()
    pl.semaphore_signal(barrier, inc=1, device_id=side, device_id_type=MESH)

    @pl.when(jnp.logical_not(is_first))
    def _():
        pl.semaphore_signal(barrier, inc=1, device_id=before, device_id_type=MESH)
        pl.semaphore_signal(barrier, inc=1, device_id=before_side, device_id_type=MESH)

    @pl.when(jnp.logical_not(is_last))
    def _():
        pl.semaphore_signal(barrier, inc=1, device_id=after, device_id_type=MESH)
        pl.semaphore_signal(barrier, inc=1, device_id=after_side, device_id_type=MESH)

    if detour:
        @pl.when(is_low_mid | is_high_mid)
        def _():
            for far_slab in (0, depth - 1):
                pl.semaphore_signal(barrier, inc=1, device_id=(far_slab, gy), device_id_type=MESH)

        @pl.when(is_first | is_last)
        def _():
            for far_slab in (middle - 1, middle):
                pl.semaphore_signal(barrier, inc=1, device_id=(far_slab, gy), device_id_type=MESH)

    lane = lax.broadcasted_iota(jnp.int32, (8, 128), 1)
    row = lax.broadcasted_iota(jnp.int32, (8, 128), 0)
    zero = jnp.zeros((8, 128), jnp.float32)
    low_half = lane < 64

    zero_row = pl.multiple_of(48 * gy, 8)
    strip_row = pl.multiple_of(48 - 48 * gy, 8)
    raw[:, :, pl.ds(zero_row, 8), :] = jnp.zeros((5, RAW_PLANES, 8, 128), jnp.float32)
    halo_sum[...] = jnp.zeros_like(halo_sum)
    main_row = pl.multiple_of(8 * gy, 8)
    edge_row = pl.multiple_of(40 - 40 * gy, 8)

    local[0].wait()
    local[1].wait()
    for z in range(PLANES):
        raw[4, HALO + z, HALO : HALO + ROWS, :] = jnp.concatenate([f_tail[z], m_tail[z]], axis=-1)
    for copy in local[2:6]:
        copy.wait()

    if detour:
        @pl.when(is_low_mid | is_high_mid)
        def _():
            pl.semaphore_wait(barrier, 7)

        @pl.when(jnp.logical_not(is_low_mid | is_high_mid))
        def _():
            pl.semaphore_wait(barrier, 5)
    else:
        @pl.when(is_first | is_last)
        def _():
            pl.semaphore_wait(barrier, 3)

        @pl.when(jnp.logical_not(is_first | is_last))
        def _():
            pl.semaphore_wait(barrier, 5)

    src_row = pl.multiple_of(40 - 32 * gy, 8)
    y_copies = []
    for i, first in enumerate(PAIRS):
        copy = pltpu.make_async_remote_copy(
            src_ref=raw.at[:, pl.ds(HALO + first, 2), pl.ds(src_row, 8), :],
            dst_ref=raw.at[:, pl.ds(HALO + first, 2), pl.ds(zero_row, 8), :],
            send_sem=y_send.at[i], recv_sem=y_recv.at[i], device_id=side, device_id_type=MESH,
        )
        copy.start()
        y_copies.append(copy)

    def plane_to_after(k, h):
        return pltpu.make_async_remote_copy(
            src_ref=raw.at[:, 17 - 2 * k - h, rows_own, :],
            dst_ref=raw.at[:, 7 - 2 * k - h, rows_own, :],
            send_sem=z_send.at[0, k, h], recv_sem=z_recv.at[0, k, h], device_id=after, device_id_type=MESH,
        )

    def plane_to_before(k, h):
        return pltpu.make_async_remote_copy(
            src_ref=raw.at[:, 8 + 2 * k + h, rows_own, :],
            dst_ref=raw.at[:, 18 + 2 * k + h, rows_own, :],
            send_sem=z_send.at[1, k, h], recv_sem=z_recv.at[1, k, h], device_id=before, device_id_type=MESH,
        )

    strip = pl.ds(strip_row, 8)

    def strip_to_after(k):
        return pltpu.make_async_remote_copy(
            src_ref=raw.at[:, pl.ds(16 - 2 * k, 2), strip, :],
            dst_ref=raw.at[:, pl.ds(6 - 2 * k, 2), strip, :],
            send_sem=s_send.at[0, k], recv_sem=s_recv.at[0, k], device_id=after, device_id_type=MESH,
        )

    def strip_to_before(k):
        return pltpu.make_async_remote_copy(
            src_ref=raw.at[:, pl.ds(8 + 2 * k, 2), strip, :],
            dst_ref=raw.at[:, pl.ds(18 + 2 * k, 2), strip, :],
            send_sem=s_send.at[1, k], recv_sem=s_recv.at[1, k], device_id=before, device_id_type=MESH,
        )

    def hop_up(i):
        (k, h), way = DETOUR[i]
        return pltpu.make_async_remote_copy(
            src_ref=raw.at[:, 17 - 2 * k - h, rows_own, :], dst_ref=passing.at[i],
            send_sem=z_send.at[0, k, h], recv_sem=hop_recv.at[i],
            device_id=((0, depth - 1)[way], gy), device_id_type=MESH,
        )

    def hop_down(i):
        (k, h), way = DETOUR[i]
        return pltpu.make_async_remote_copy(
            src_ref=raw.at[:, 8 + 2 * k + h, rows_own, :], dst_ref=passing.at[i],
            send_sem=z_send.at[1, k, h], recv_sem=hop_recv.at[i],
            device_id=((depth - 1, 0)[way], gy), device_id_type=MESH,
        )

    def on_up(i):
        (k, h), way = DETOUR[i]
        return pltpu.make_async_remote_copy(
            src_ref=passing.at[i], dst_ref=raw.at[:, 7 - 2 * k - h, rows_own, :],
            send_sem=hop_send.at[i], recv_sem=z_recv.at[0, k, h], device_id=(middle, gy), device_id_type=MESH,
        )

    def on_down(i):
        (k, h), way = DETOUR[i]
        return pltpu.make_async_remote_copy(
            src_ref=passing.at[i], dst_ref=raw.at[:, 18 + 2 * k + h, rows_own, :],
            send_sem=hop_send.at[i], recv_sem=z_recv.at[1, k, h], device_id=(middle - 1, gy), device_id_type=MESH,
        )

    sends_up = jnp.logical_not(is_last)
    sends_down = jnp.logical_not(is_first)

    def start_plane(k, h):
        goes_round = (k, h) in ROUND
        up = sends_up & jnp.logical_not(is_low_mid) if goes_round else sends_up
        down = sends_down & jnp.logical_not(is_high_mid) if goes_round else sends_down

        @pl.when(up)
        def _():
            plane_to_after(k, h).start()

        @pl.when(down)
        def _():
            plane_to_before(k, h).start()

    def start_strips(k):
        @pl.when(sends_up)
        def _():
            strip_to_after(k).start()

        @pl.when(sends_down)
        def _():
            strip_to_before(k).start()

    def start_hop(i):
        @pl.when(is_low_mid)
        def _():
            hop_up(i).start()

        @pl.when(is_high_mid)
        def _():
            hop_down(i).start()

    def pass_on(i):
        if detour and i < len(DETOUR):
            way = DETOUR[i][1]

            @pl.when((is_first, is_last)[way])
            def _():
                hop_up(i).wait_recv()
                on_up(i).start()

            @pl.when((is_last, is_first)[way])
            def _():
                hop_down(i).wait_recv()
                on_down(i).start()

    def wait_planes(k, h):
        @pl.when(sends_down)
        def _():
            plane_to_after(k, h).wait_recv()

        @pl.when(sends_up)
        def _():
            plane_to_before(k, h).wait_recv()

    def wait_strips(k):
        @pl.when(sends_down)
        def _():
            strip_to_after(k).wait_recv()

        @pl.when(sends_up)
        def _():
            strip_to_before(k).wait_recv()

    for k, h in ((0, 0), (0, 1), (1, 0), (1, 1), (2, 0), (2, 1), (3, 0), (3, 1)):
        if (k, h) < (2, 1):
            start_plane(k, h)
        if detour and (k, h) in ROUND:
            start_hop(ROUND.index((k, h)))

    @pl.when(is_first)
    def _():
        raw[:, 0:HALO, :, :] = jnp.zeros((5, HALO, RAW_ROWS, 128), jnp.float32)

    @pl.when(is_last)
    def _():
        raw[:, HALO + PLANES : RAW_PLANES, :, :] = jnp.zeros((5, HALO, RAW_ROWS, 128), jnp.float32)

    def fields_of(plane, rows):
        out = []
        for t in range(2):
            f = raw[t, plane, rows, :]
            m = raw[2 + t, plane, rows, :]
            out += [f, m, f * f, m * m, f * m]
        p = raw[4, plane, rows, :]
        return out + [p, p * p, p * pltpu.roll(p, 64, 1)]

    def own_windows(rows):
        columns = [fields_of(HALO + z, rows) for z in range(PLANES)]
        for col in range(13):
            values = [columns[z][col] for z in range(PLANES)]
            for p, total in enumerate(prefix_sums(values[:9])):
                own_sum[col, p, rows, :] = total
            for p, total in enumerate(suffix_sums(values[1:])):
                own_sum[col, 9 + p, rows, :] = total

    @pl.loop(0, 6)
    def _(i):
        own_windows(pl.ds(pl.multiple_of(main_row + 8 * i, 8), 8))

    def coefficients(items, base, count, part):
        offset = 48 * part
        for n, (plane, halo, side_of) in enumerate(items):
            for g in range(count + 1):
                rows = pl.ds(pl.multiple_of(base + 8 * g, 8), 8)
                here = pl.ds(8 * g, 8)
                if halo is None:
                    for col in range(13):
                        zsum[13 * n + col, here, :] = own_sum[col, plane, rows, :]
                else:
                    there = pl.ds(offset + 8 * g, 8)
                    fields = fields_of(halo, rows)
                    for col in range(13):
                        total = halo_sum[side_of, col, there, :] + fields[col]
                        halo_sum[side_of, col, there, :] = total
                        zsum[13 * n + col, here, :] = total + own_sum[col, plane, rows, :]
        for n in range(len(items)):
            for col in range(13):
                at = 13 * n + col
                for g in range(count + 1):
                    ysum[at, pl.ds(8 * g, 8), :] = (
                        zsum[at, pl.ds(8 * g, 8), :] + zsum[at, pl.ds(8 * g + 1, 8), :] + zsum[at, pl.ds(8 * g + 2, 8), :]
                    )
                for j in range(count):
                    total = (
                        ysum[at, pl.ds(8 * j, 8), :] + ysum[at, pl.ds(8 * j + 3, 8), :] + ysum[at, pl.ds(8 * j + 6, 8), :]
                    )
                    if col < 10:
                        stage_y[n, j, 3 * (col % 5) + col // 5] = total
                    elif col == 12:
                        stage_y[n, j, 14] = jnp.where(low_half, total, 0.0)
                    else:
                        stage_y[n, j, 6 * (col - 10) + 2] = jnp.where(low_half, total, 0.0)
                        stage_y[n, j, 6 * (col - 10) + 5] = jnp.where(low_half, pltpu.roll(total, 64, 1), 0.0)
        for n in range(len(items)):
            for j in range(count):
                for i in range(5):
                    three = three_along_x([stage_y[n, j, 3 * i + t] for t in range(3)], 1, lane)
                    for t in range(3):
                        stage_x[n, j, 3 * i + t] = three[t]
        for n, (plane, halo, side_of) in enumerate(items):
            position = gz * PLANES + plane - RADIUS
            inside = (position >= 0) & (position < depth * PLANES)
            for j in range(count):
                boxed = [three_along_x([stage_x[n, j, 3 * i + t] for t in range(3)], 3, lane) for i in range(5)]
                position = base + 8 * j + row + 40 * gy - RADIUS
                valid = jnp.where(inside & (position >= 0) & (position < 80), 1.0, 0.0)
                where = pl.ds(pl.multiple_of(base + 8 * j, 8), 8)
                for t in range(3):
                    sf, sm, sff, smm, sfm = [boxed[i][t] for i in range(5)]
                    mf = sf * (1.0 / WINDOW)
                    mm = sm * (1.0 / WINDOW)
                    a = (sfm - mf * sm) * (valid if t < 2 else jnp.where(low_half, valid, 0.0))
                    p = sff - mf * sf + EPS
                    q = smm - mm * sm + EPS
                    r = 1.0 / (p * q)
                    cross = a * r
                    moving = -cross * a * (r * p)
                    for i, value in enumerate((cross, moving, cross * mf + moving * mm)):
                        if halo is not None:
                            value = value + coef[3 * i + t, plane + (1, -1)[side_of], where, :]
                        coef[3 * i + t, plane, where, :] = value

    middle_items = [(8, None, 0), (9, None, 1)]

    def step_items(step):
        return [(7 - step, 7 - step, 0), (10 + step, 18 + step, 1)]

    def main_part(items):
        coefficients(items, main_row, 5, 0)

    def edge_part(items):
        coefficients(items, edge_row, 1, 1)

    def slope_planes(planes, ends):
        for s, z in enumerate(planes):
            for col in range(9):
                values = []
                for m in range(13):
                    where = pl.ds(m, 8, stride=5)
                    if ends:
                        values.append(coef[col, (0, COEF_PLANES - 1)[s], where, :])
                    else:
                        values.append(coef[col, z, where, :] + coef[col, z + 2 * RADIUS, where, :])
                total = windows_of_nine(values)
                for j in range(5):
                    stage_y[s, j, col] = total[j]
        for s in range(2):
            for j in range(5):
                for i in range(3):
                    three = three_along_x([stage_y[s, j, 3 * i + t] for t in range(3)], 1, lane)
                    for t in range(3):
                        stage_x[s, j, 3 * i + t] = three[t]
        for s, z in enumerate(planes):
            for j in range(5):
                boxed = [three_along_x([stage_x[s, j, 3 * i + t] for t in range(3)], 3, lane) for i in range(3)]
                centre = pl.ds(HALO + j, 8, stride=5)
                tail = raw[4, HALO + z, centre, :]
                f = [raw[0, HALO + z, centre, :], raw[1, HALO + z, centre, :], tail]
                m = [raw[2, HALO + z, centre, :], raw[3, HALO + z, centre, :], pltpu.roll(tail, 64, 1)]
                for t in range(3):
                    slope = f[t] * boxed[0][t] + m[t] * boxed[1][t] - boxed[2][t]
                    for c in range(3):
                        weighted[c, t, j, z] = slope * grad[t, c, z, pl.ds(j, 8, stride=5), :]

    main_part(middle_items)

    for copy in local[6:]:
        copy.wait()
    grad[2] = jnp.concatenate([g_tail[...], jnp.zeros_like(g_tail)], axis=-1)

    @pl.loop(0, 7)
    def _(step):
        wait_planes(step // 2, step % 2)
        main_part(step_items(step))

        for after_step in sorted(set(PASS_AFTER)):
            @pl.when(step == after_step)
            def _():
                for i, when in enumerate(PASS_AFTER):
                    if when == after_step:
                        pass_on(i)

        @pl.when(step == 1)
        def _():
            y_copies[0].wait_recv()
            y_copies[1].wait_recv()
            start_strips(0)
            start_plane(2, 1)
            start_plane(3, 0)

        @pl.when(step == 2)
        def _():
            y_copies[2].wait_recv()
            y_copies[3].wait_recv()
            start_strips(1)

        @pl.when(step == 3)
        def _():
            y_copies[4].wait_recv()
            start_strips(2)
            start_strips(3)
            start_plane(3, 1)
            own_windows(strip)

        @pl.when(step == 5)
        def _():
            wait_strips(0)
            wait_strips(1)
            edge_part(middle_items + step_items(0) + step_items(1) + step_items(2))

    wait_strips(2)
    wait_strips(3)
    edge_part(step_items(3) + step_items(4) + step_items(5) + step_items(6))

    @pl.loop(3, 7)
    def _(step):
        slope_planes((7 - step, 2 + step), False)

    wy = [spline_weights(j) for j in range(SPACING)]
    wz = [[-2.0 * SIM_WEIGHT * w for w in ws] for ws in wy]

    def add_plane(slots, z, value):
        for k in range(4):
            weight = wz[z % SPACING][k]
            if weight != 0.0:
                m = z // SPACING + k
                slots[m] = weight * value if slots[m] is None else slots[m] + weight * value

    for t in range(3):
        @pl.loop(0, 3)
        def _(c):
            for j in range(SPACING):
                slots = [None] * 5
                for z in range(1, PLANES - 1):
                    add_plane(slots, z, weighted[c, t, j, z])
                for m in range(5):
                    inner_sum[c, t, j, m] = slots[m]

    wait_planes(3, 1)
    main_part(step_items(7))
    edge_part(step_items(7))
    slope_planes((0, PLANES - 1), True)

    for t in range(3):
        @pl.loop(0, 3)
        def _(c):
            slots = []
            for j in range(SPACING):
                parts = [inner_sum[c, t, j, m] for m in range(5)]
                add_plane(parts, 0, weighted[c, t, j, 0])
                add_plane(parts, PLANES - 1, weighted[c, t, j, PLANES - 1])
                slots.append(parts)
            for m in range(5):
                y = []
                for k in range(4):
                    total = wy[0][k] * slots[0][m]
                    for j in range(1, SPACING):
                        total = total + wy[j][k] * slots[j][m]
                    y.append(total)
                r0, r2, r3 = pltpu.roll(y[0], 7, 0), pltpu.roll(y[2], 1, 0), pltpu.roll(y[3], 2, 0)
                inner = (
                    jnp.where(row == 7, 0.0, r0) + y[1] + jnp.where(row == 0, 0.0, r2) + jnp.where(row < 2, 0.0, r3)
                )
                to_low = jnp.where(row == 7, r0, 0.0)
                to_high = jnp.where(row == 0, r2, 0.0) + jnp.where(row < 2, r3, 0.0)
                clip_low = jnp.where(row == 0, y[0], 0.0)
                clip_high = jnp.where(row == 7, y[2] + y[3] + pltpu.roll(y[3], 1, 0), 0.0)
                is_low = gy == 0
                base = pl.multiple_of(48 * m + 8 * c, 8)
                lanes = pl.ds(128 * t, 128)
                wide[pl.ds(base, 8), lanes] = inner + jnp.where(is_low, clip_low, clip_high)
                wide[pl.ds(pl.multiple_of(base + 24, 8), 8), lanes] = jnp.where(is_low, to_high, to_low)

    left = wide[...]
    high = left.astype(jnp.bfloat16)
    low = (left - high.astype(jnp.float32)).astype(jnp.bfloat16)

    def dot(a, b):
        return jnp.dot(a, b, preferred_element_type=jnp.float32)

    total = dot(high, bh[...]) + (dot(low, bh[...]) + dot(high, bl[...]))
    sums[...] = total.reshape(5, 2, 3, 8, 128)

    copies = [
        (0, sums.at[0, 0], from_next, before, 0),
        (0, sums.at[0, 1], from_next_side, before_side, 1),
        (1, sums.at[pl.ds(3, 2), 0], from_prev, after, 2),
        (1, sums.at[pl.ds(3, 2), 1], from_prev_side, after_side, 3),
    ]
    rdmas = [
        (
            direction,
            pltpu.make_async_remote_copy(
                src_ref=src, dst_ref=dst, send_sem=e_send.at[i], recv_sem=e_recv.at[i],
                device_id=target, device_id_type=MESH,
            ),
        )
        for direction, src, dst, target, i in copies
    ]
    side_copy = pltpu.make_async_remote_copy(
        src_ref=sums.at[pl.ds(1, 2), 1], dst_ref=from_side, send_sem=e_send.at[4], recv_sem=e_recv.at[4],
        device_id=side, device_id_type=MESH,
    )

    @pl.when(jnp.logical_not(is_first))
    def _():
        for direction, copy in rdmas:
            if direction == 0:
                copy.start()

    @pl.when(jnp.logical_not(is_last))
    def _():
        for direction, copy in rdmas:
            if direction == 1:
                copy.start()

    low_clip = jnp.where(is_first, 1.0, 0.0)
    high_clip = jnp.where(is_last, 1.0, 0.0)
    sums[1] = sums[1] + low_clip * sums[0]
    sums[2] = sums[2] + high_clip * (sums[3] + sums[4])
    side_copy.start()

    @pl.when(is_last)
    def _():
        from_next[...] = jnp.zeros_like(from_next)
        from_next_side[...] = jnp.zeros_like(from_next_side)

    @pl.when(is_first)
    def _():
        from_prev[...] = jnp.zeros_like(from_prev)
        from_prev_side[...] = jnp.zeros_like(from_prev_side)

    @pl.when(jnp.logical_not(is_last))
    def _():
        for direction, copy in rdmas:
            if direction == 0:
                copy.wait_recv()

    @pl.when(jnp.logical_not(is_first))
    def _():
        for direction, copy in rdmas:
            if direction == 1:
                copy.wait_recv()

    side_copy.wait_recv()
    first = sums[1, 0] + from_side[0] + from_prev[0] + from_prev_side[0]
    second = sums[2, 0] + from_side[1] + from_prev[1] + from_prev_side[1] + from_next[...] + from_next_side[...]
    out_ref[0] = first[:, :, :POINTS]
    out_ref[1] = second[:, :, :POINTS]

    for copy in y_copies:
        copy.wait_send()
    for k in range(4):
        @pl.when(sends_up)
        def _():
            plane_to_after(k, 0).wait_send()
            plane_to_after(k, 1).wait_send()
            strip_to_after(k).wait_send()

        @pl.when(sends_down)
        def _():
            plane_to_before(k, 0).wait_send()
            plane_to_before(k, 1).wait_send()
            strip_to_before(k).wait_send()

    if detour:
        @pl.when(is_first | is_last)
        def _():
            for i in range(len(DETOUR)):
                on_up(i).wait_send()

    side_copy.wait_send()

    @pl.when(jnp.logical_not(is_first))
    def _():
        for direction, copy in rdmas:
            if direction == 0:
                copy.wait_send()

    @pl.when(jnp.logical_not(is_last))
    def _():
        for direction, copy in rdmas:
            if direction == 1:
                copy.wait_send()


def local_gradient(depth, fixed_image, moving_image, moving_grad):
    high, low = basis_along_x()
    f32 = jnp.float32
    anywhere = pl.BlockSpec(memory_space=pl.ANY)
    dma = pltpu.SemaphoreType.DMA
    return pl.pallas_call(
        functools.partial(kernel, depth),
        out_shape=jax.ShapeDtypeStruct((2, 3, 8, POINTS), f32),
        in_specs=[anywhere] * 5,
        out_specs=pl.BlockSpec(memory_space=pltpu.VMEM),
        scratch_shapes=[
            pltpu.VMEM((5, RAW_PLANES, RAW_ROWS, 128), f32),
            pltpu.VMEM((PLANES, ROWS, 64), f32),
            pltpu.VMEM((PLANES, ROWS, 64), f32),
            pltpu.VMEM((3, 3, PLANES, ROWS, 128), f32),
            pltpu.VMEM((3, PLANES, ROWS, 64), f32),
            pltpu.VMEM((384, 128), jnp.bfloat16),
            pltpu.VMEM((384, 128), jnp.bfloat16),
            pltpu.VMEM((13, COEF_PLANES, RAW_ROWS, 128), f32),
            pltpu.VMEM((2, 13, 64, 128), f32),
            pltpu.VMEM((104, RAW_ROWS, 128), f32),
            pltpu.VMEM((104, RAW_ROWS, 128), f32),
            pltpu.VMEM((8, 5, 15, 8, 128), f32),
            pltpu.VMEM((8, 5, 15, 8, 128), f32),
            pltpu.VMEM((9, COEF_PLANES, COEF_ROWS, 128), f32),
            pltpu.VMEM((3, 3, 5, PLANES, 8, 128), f32),
            pltpu.VMEM((3, 3, 5, 5, 8, 128), f32),
            pltpu.VMEM((240, 384), f32),
            pltpu.VMEM((5, 2, 3, 8, 128), f32),
            pltpu.VMEM((4, 5, ROWS, 128), f32),
            pltpu.VMEM((3, 8, 128), f32),
            pltpu.VMEM((2, 3, 8, 128), f32),
            pltpu.VMEM((2, 3, 8, 128), f32),
            pltpu.VMEM((3, 8, 128), f32),
            pltpu.VMEM((2, 3, 8, 128), f32),
            dma((11,)),
            dma((5,)),
            dma((5,)),
            dma((2, 4, 2)),
            dma((2, 4, 2)),
            dma((2, 4)),
            dma((2, 4)),
            dma((4,)),
            dma((4,)),
            dma((5,)),
            dma((5,)),
        ],
        compiler_params=pltpu.CompilerParams(collective_id=0, has_side_effects=True, vmem_limit_bytes=56500000),
    )(fixed_image, moving_image, moving_grad, high, low)


def solution(mesh):
    in_specs = (P("gz", "gy", None), P("gz", "gy", None), P(None, "gz", "gy", None))
    out_specs = P("gz", None, "gy", None)
    body = functools.partial(local_gradient, mesh.shape["gz"])
    return jax.shard_map(body, mesh=mesh, in_specs=in_specs, out_specs=out_specs, check_vma=False)
```

```python
import functools

import jax
import jax.numpy as jnp
import numpy as np
from jax import lax
from jax.experimental import pallas as pl
from jax.experimental.pallas import tpu as pltpu
from jax.sharding import PartitionSpec as P

RADIUS = 4
SPACING = 5
EPS = 36.0
SIM_WEIGHT = 8.0
WINDOW = float((2 * RADIUS + 1) ** 3)
MESH = pl.DeviceIdType.MESH

PLANES = 10
ROWS = 40
NX = 320
POINTS = 64
HALO = 2 * RADIUS
RAW_PLANES = PLANES + 2 * HALO
RAW_ROWS = ROWS + 2 * HALO
COEF_PLANES = PLANES + 2 * RADIUS
COEF_ROWS = ROWS + 2 * RADIUS
PAIRS = (0, 8, 2, 6, 4)
DETOUR = (((2, 1), 1), ((3, 0), 0), ((3, 1), 0))
PASS_AFTER = (4, 5, 6)
RELAY_AFTER = (2, 3, 4)
LATER = ((), ((3, 1),), ())
ROUND = tuple(plane for plane, way in DETOUR)


def spline_weights(step):
    u = step / SPACING
    return (
        (1.0 - u) ** 3 / 6.0,
        (3.0 * u**3 - 6.0 * u**2 + 4.0) / 6.0,
        (-3.0 * u**3 + 3.0 * u**2 + 3.0 * u + 1.0) / 6.0,
        u**3 / 6.0,
    )


def basis_along_x():
    matrix = np.zeros((384, 128), np.float64)
    for x in range(NX):
        for k, weight in enumerate(spline_weights(x % SPACING)):
            point = min(max(x // SPACING - 1 + k, 0), POINTS - 1)
            matrix[x, point] += weight
    matrix = matrix.astype(np.float32)
    high = matrix.astype(jnp.bfloat16)
    low = (matrix - high.astype(np.float32)).astype(jnp.bfloat16)
    return high, low


def suffix_sums(values):
    sums = [values[-1]]
    for value in reversed(values[:-1]):
        sums.append(sums[-1] + value)
    return sums[::-1]


def prefix_sums(values):
    sums = [values[0]]
    for value in values[1:]:
        sums.append(sums[-1] + value)
    return sums


def windows_of_nine(values):
    count = len(values) - 8
    if count > 9:
        before = suffix_sums(values[:9])
        after = prefix_sums(values[9:])
        return [before[0]] + [before[i] + after[i - 1] for i in range(1, 9)] + [after[8]]
    common = values[count - 1]
    for value in values[count:9]:
        common = common + value
    before = suffix_sums(values[: count - 1])
    after = prefix_sums(values[9:])
    out = []
    for i in range(count):
        total = common
        if i < count - 1:
            total = total + before[i]
        if i > 0:
            total = total + after[i - 1]
        out.append(total)
    return out


def three_along_x(tiles, reach, lane):
    right = [pltpu.roll(tile, reach, 1) for tile in tiles]
    left = [pltpu.roll(tile, 128 - reach, 1) for tile in tiles]
    out = []
    for i in range(3):
        before = jnp.where(lane < reach, right[i - 1], right[i])
        after = jnp.where(lane >= 128 - reach, left[(i + 1) % 3], left[i])
        out.append(tiles[i] + before + after)
    return out


def kernel(
    depth, f_hbm, m_hbm, g_hbm, bh_hbm, bl_hbm, out_ref,
    raw, f_tail, m_tail, grad, g_tail, bh, bl, own_sum, halo_sum, zsum, ysum, stage_y, stage_x, coef, weighted, inner_sum, wide,
    sums, passing, from_next, from_prev, from_side, from_next_side, from_prev_side,
    local_sem, y_send, y_recv, z_send, z_recv, s_send, s_recv, hop_send, hop_recv, e_send, e_recv,
):
    gz = lax.axis_index("gz")
    gy = lax.axis_index("gy")
    other = 1 - gy
    is_first = gz == 0
    is_last = gz == depth - 1
    before = (jnp.maximum(gz - 1, 0), gy)
    after = (jnp.minimum(gz + 1, depth - 1), gy)
    before_side = (jnp.maximum(gz - 1, 0), other)
    after_side = (jnp.minimum(gz + 1, depth - 1), other)
    side = (gz, other)
    middle = depth // 2
    detour = depth >= 4 and len(DETOUR) > 0
    is_low_mid = (gz == middle - 1) if detour else (gz < 0)
    is_high_mid = (gz == middle) if detour else (gz < 0)

    local = []

    def bring(src, dst):
        copy = pltpu.make_async_copy(src, dst, local_sem.at[len(local)])
        copy.start()
        local.append(copy)

    own = pl.ds(HALO, PLANES)
    rows_own = pl.ds(HALO, ROWS)
    bring(f_hbm.at[:, :, pl.ds(256, 64)], f_tail)
    bring(m_hbm.at[:, :, pl.ds(256, 64)], m_tail)
    for t in range(2):
        bring(f_hbm.at[:, :, pl.ds(128 * t, 128)], raw.at[t, own, rows_own, :])
        bring(m_hbm.at[:, :, pl.ds(128 * t, 128)], raw.at[2 + t, own, rows_own, :])
    for t in range(2):
        bring(g_hbm.at[:, :, :, pl.ds(128 * t, 128)], grad.at[t])
    bring(g_hbm.at[:, :, :, pl.ds(256, 64)], g_tail)
    bring(bh_hbm, bh)
    bring(bl_hbm, bl)

    barrier = pltpu.get_barrier_semaphore()
    pl.semaphore_signal(barrier, inc=1, device_id=side, device_id_type=MESH)

    @pl.when(jnp.logical_not(is_first))
    def _():
        pl.semaphore_signal(barrier, inc=1, device_id=before, device_id_type=MESH)
        pl.semaphore_signal(barrier, inc=1, device_id=before_side, device_id_type=MESH)

    @pl.when(jnp.logical_not(is_last))
    def _():
        pl.semaphore_signal(barrier, inc=1, device_id=after, device_id_type=MESH)
        pl.semaphore_signal(barrier, inc=1, device_id=after_side, device_id_type=MESH)

    if detour:
        @pl.when(is_low_mid | is_high_mid)
        def _():
            for far_slab in (0, depth - 1):
                pl.semaphore_signal(barrier, inc=1, device_id=(far_slab, gy), device_id_type=MESH)

        @pl.when(is_first | is_last)
        def _():
            for far_slab in (middle - 1, middle):
                pl.semaphore_signal(barrier, inc=1, device_id=(far_slab, gy), device_id_type=MESH)

    lane = lax.broadcasted_iota(jnp.int32, (8, 128), 1)
    row = lax.broadcasted_iota(jnp.int32, (8, 128), 0)
    zero = jnp.zeros((8, 128), jnp.float32)
    low_half = lane < 64

    zero_row = pl.multiple_of(48 * gy, 8)
    strip_row = pl.multiple_of(48 - 48 * gy, 8)
    raw[:, :, pl.ds(zero_row, 8), :] = jnp.zeros((5, RAW_PLANES, 8, 128), jnp.float32)
    halo_sum[...] = jnp.zeros_like(halo_sum)
    main_row = pl.multiple_of(8 * gy, 8)
    edge_row = pl.multiple_of(40 - 40 * gy, 8)

    local[0].wait()
    local[1].wait()
    for z in range(PLANES):
        raw[4, HALO + z, HALO : HALO + ROWS, :] = jnp.concatenate([f_tail[z], m_tail[z]], axis=-1)
    for copy in local[2:6]:
        copy.wait()

    if detour:
        @pl.when(is_low_mid | is_high_mid)
        def _():
            pl.semaphore_wait(barrier, 7)

        @pl.when(jnp.logical_not(is_low_mid | is_high_mid))
        def _():
            pl.semaphore_wait(barrier, 5)
    else:
        @pl.when(is_first | is_last)
        def _():
            pl.semaphore_wait(barrier, 3)

        @pl.when(jnp.logical_not(is_first | is_last))
        def _():
            pl.semaphore_wait(barrier, 5)

    src_row = pl.multiple_of(40 - 32 * gy, 8)
    y_copies = []
    for i, first in enumerate(PAIRS):
        copy = pltpu.make_async_remote_copy(
            src_ref=raw.at[:, pl.ds(HALO + first, 2), pl.ds(src_row, 8), :],
            dst_ref=raw.at[:, pl.ds(HALO + first, 2), pl.ds(zero_row, 8), :],
            send_sem=y_send.at[i], recv_sem=y_recv.at[i], device_id=side, device_id_type=MESH,
        )
        copy.start()
        y_copies.append(copy)

    def plane_to_after(k, h):
        return pltpu.make_async_remote_copy(
            src_ref=raw.at[:, 17 - 2 * k - h, rows_own, :],
            dst_ref=raw.at[:, 7 - 2 * k - h, rows_own, :],
            send_sem=z_send.at[0, k, h], recv_sem=z_recv.at[0, k, h], device_id=after, device_id_type=MESH,
        )

    def plane_to_before(k, h):
        return pltpu.make_async_remote_copy(
            src_ref=raw.at[:, 8 + 2 * k + h, rows_own, :],
            dst_ref=raw.at[:, 18 + 2 * k + h, rows_own, :],
            send_sem=z_send.at[1, k, h], recv_sem=z_recv.at[1, k, h], device_id=before, device_id_type=MESH,
        )

    strip = pl.ds(strip_row, 8)

    def strip_to_after(k):
        return pltpu.make_async_remote_copy(
            src_ref=raw.at[:, pl.ds(16 - 2 * k, 2), strip, :],
            dst_ref=raw.at[:, pl.ds(6 - 2 * k, 2), strip, :],
            send_sem=s_send.at[0, k], recv_sem=s_recv.at[0, k], device_id=after, device_id_type=MESH,
        )

    def strip_to_before(k):
        return pltpu.make_async_remote_copy(
            src_ref=raw.at[:, pl.ds(8 + 2 * k, 2), strip, :],
            dst_ref=raw.at[:, pl.ds(18 + 2 * k, 2), strip, :],
            send_sem=s_send.at[1, k], recv_sem=s_recv.at[1, k], device_id=before, device_id_type=MESH,
        )

    def hop_up(i):
        (k, h), way = DETOUR[i]
        return pltpu.make_async_remote_copy(
            src_ref=raw.at[:, 17 - 2 * k - h, rows_own, :], dst_ref=passing.at[i],
            send_sem=z_send.at[0, k, h], recv_sem=hop_recv.at[i],
            device_id=((0, depth - 1)[way], gy), device_id_type=MESH,
        )

    def hop_down(i):
        (k, h), way = DETOUR[i]
        return pltpu.make_async_remote_copy(
            src_ref=raw.at[:, 8 + 2 * k + h, rows_own, :], dst_ref=passing.at[i],
            send_sem=z_send.at[1, k, h], recv_sem=hop_recv.at[i],
            device_id=((depth - 1, 0)[way], gy), device_id_type=MESH,
        )

    def on_up(i):
        (k, h), way = DETOUR[i]
        return pltpu.make_async_remote_copy(
            src_ref=passing.at[i], dst_ref=raw.at[:, 7 - 2 * k - h, rows_own, :],
            send_sem=hop_send.at[i], recv_sem=z_recv.at[0, k, h], device_id=(middle, gy), device_id_type=MESH,
        )

    def on_down(i):
        (k, h), way = DETOUR[i]
        return pltpu.make_async_remote_copy(
            src_ref=passing.at[i], dst_ref=raw.at[:, 18 + 2 * k + h, rows_own, :],
            send_sem=hop_send.at[i], recv_sem=z_recv.at[1, k, h], device_id=(middle - 1, gy), device_id_type=MESH,
        )

    sends_up = jnp.logical_not(is_last)
    sends_down = jnp.logical_not(is_first)

    def start_plane(k, h):
        goes_round = (k, h) in ROUND
        up = sends_up & jnp.logical_not(is_low_mid) if goes_round else sends_up
        down = sends_down & jnp.logical_not(is_high_mid) if goes_round else sends_down

        @pl.when(up)
        def _():
            plane_to_after(k, h).start()

        @pl.when(down)
        def _():
            plane_to_before(k, h).start()

    def start_strips(k):
        @pl.when(sends_up)
        def _():
            strip_to_after(k).start()

        @pl.when(sends_down)
        def _():
            strip_to_before(k).start()

    def start_hop(i):
        @pl.when(is_low_mid)
        def _():
            hop_up(i).start()

        @pl.when(is_high_mid)
        def _():
            hop_down(i).start()

    def pass_on(i):
        if detour and i < len(DETOUR):
            way = DETOUR[i][1]

            @pl.when((is_first, is_last)[way])
            def _():
                hop_up(i).wait_recv()
                on_up(i).start()

            @pl.when((is_last, is_first)[way])
            def _():
                hop_down(i).wait_recv()
                on_down(i).start()

    def wait_planes(k, h):
        @pl.when(sends_down)
        def _():
            plane_to_after(k, h).wait_recv()

        @pl.when(sends_up)
        def _():
            plane_to_before(k, h).wait_recv()

    def wait_strips(k):
        @pl.when(sends_down)
        def _():
            strip_to_after(k).wait_recv()

        @pl.when(sends_up)
        def _():
            strip_to_before(k).wait_recv()

    for k, h in ((0, 0), (0, 1), (1, 0), (1, 1), (2, 0), (2, 1), (3, 0), (3, 1)):
        if (k, h) < (3, 1):
            start_plane(k, h)
        if detour and (k, h) in ROUND:
            start_hop(ROUND.index((k, h)))

    @pl.when(is_first)
    def _():
        raw[:, 0:HALO, :, :] = jnp.zeros((5, HALO, RAW_ROWS, 128), jnp.float32)

    @pl.when(is_last)
    def _():
        raw[:, HALO + PLANES : RAW_PLANES, :, :] = jnp.zeros((5, HALO, RAW_ROWS, 128), jnp.float32)

    def fields_of(plane, rows):
        out = []
        for t in range(2):
            f = raw[t, plane, rows, :]
            m = raw[2 + t, plane, rows, :]
            out += [f, m, f * f, m * m, f * m]
        p = raw[4, plane, rows, :]
        return out + [p, p * p, p * pltpu.roll(p, 64, 1)]

    def own_windows(rows):
        columns = [fields_of(HALO + z, rows) for z in range(PLANES)]
        for col in range(13):
            values = [columns[z][col] for z in range(PLANES)]
            for p, total in enumerate(prefix_sums(values[:9])):
                own_sum[col, p, rows, :] = total
            for p, total in enumerate(suffix_sums(values[1:])):
                own_sum[col, 9 + p, rows, :] = total

    @pl.loop(0, 6)
    def _(i):
        own_windows(pl.ds(pl.multiple_of(main_row + 8 * i, 8), 8))

    def coefficients(items, base, count, part, first=0):
        offset = 48 * part
        for n, (plane, halo, side_of) in enumerate(items, first):
            for g in range(count + 1):
                rows = pl.ds(pl.multiple_of(base + 8 * g, 8), 8)
                here = pl.ds(8 * g, 8)
                if halo is None:
                    for col in range(13):
                        zsum[13 * n + col, here, :] = own_sum[col, plane, rows, :]
                else:
                    there = pl.ds(offset + 8 * g, 8)
                    fields = fields_of(halo, rows)
                    for col in range(13):
                        total = halo_sum[side_of, col, there, :] + fields[col]
                        halo_sum[side_of, col, there, :] = total
                        zsum[13 * n + col, here, :] = total + own_sum[col, plane, rows, :]
        for n in range(first, first + len(items)):
            for col in range(13):
                at = 13 * n + col
                for g in range(count + 1):
                    ysum[at, pl.ds(8 * g, 8), :] = (
                        zsum[at, pl.ds(8 * g, 8), :] + zsum[at, pl.ds(8 * g + 1, 8), :] + zsum[at, pl.ds(8 * g + 2, 8), :]
                    )
                for j in range(count):
                    total = (
                        ysum[at, pl.ds(8 * j, 8), :] + ysum[at, pl.ds(8 * j + 3, 8), :] + ysum[at, pl.ds(8 * j + 6, 8), :]
                    )
                    if col < 10:
                        stage_y[n, j, 3 * (col % 5) + col // 5] = total
                    elif col == 12:
                        stage_y[n, j, 14] = jnp.where(low_half, total, 0.0)
                    else:
                        stage_y[n, j, 6 * (col - 10) + 2] = jnp.where(low_half, total, 0.0)
                        stage_y[n, j, 6 * (col - 10) + 5] = jnp.where(low_half, pltpu.roll(total, 64, 1), 0.0)
        for n in range(first, first + len(items)):
            for j in range(count):
                for i in range(5):
                    three = three_along_x([stage_y[n, j, 3 * i + t] for t in range(3)], 1, lane)
                    for t in range(3):
                        stage_x[n, j, 3 * i + t] = three[t]
        for n, (plane, halo, side_of) in enumerate(items, first):
            position = gz * PLANES + plane - RADIUS
            inside = (position >= 0) & (position < depth * PLANES)
            for j in range(count):
                boxed = [three_along_x([stage_x[n, j, 3 * i + t] for t in range(3)], 3, lane) for i in range(5)]
                position = base + 8 * j + row + 40 * gy - RADIUS
                valid = jnp.where(inside & (position >= 0) & (position < 80), 1.0, 0.0)
                where = pl.ds(pl.multiple_of(base + 8 * j, 8), 8)
                for t in range(3):
                    sf, sm, sff, smm, sfm = [boxed[i][t] for i in range(5)]
                    mf = sf * (1.0 / WINDOW)
                    mm = sm * (1.0 / WINDOW)
                    a = (sfm - mf * sm) * (valid if t < 2 else jnp.where(low_half, valid, 0.0))
                    p = sff - mf * sf + EPS
                    q = smm - mm * sm + EPS
                    r = 1.0 / (p * q)
                    cross = a * r
                    moving = -cross * a * (r * p)
                    for i, value in enumerate((cross, moving, cross * mf + moving * mm)):
                        if halo is not None:
                            value = value + coef[3 * i + t, plane + (1, -1)[side_of], where, :]
                        coef[3 * i + t, plane, where, :] = value

    middle_items = [(8, None, 0), (9, None, 1)]

    def step_items(step):
        return [(7 - step, 7 - step, 0), (10 + step, 18 + step, 1)]

    def main_part(items):
        coefficients(items, main_row, 5, 0)

    def edge_part(items, first=0):
        coefficients(items, edge_row, 1, 1, first)

    def slope_planes(planes, ends):
        for s, z in enumerate(planes):
            for col in range(9):
                values = []
                for m in range(13):
                    where = pl.ds(m, 8, stride=5)
                    if ends:
                        values.append(coef[col, (0, COEF_PLANES - 1)[s], where, :])
                    else:
                        values.append(coef[col, z, where, :] + coef[col, z + 2 * RADIUS, where, :])
                total = windows_of_nine(values)
                for j in range(5):
                    stage_y[s, j, col] = total[j]
        for s in range(2):
            for j in range(5):
                for i in range(3):
                    three = three_along_x([stage_y[s, j, 3 * i + t] for t in range(3)], 1, lane)
                    for t in range(3):
                        stage_x[s, j, 3 * i + t] = three[t]
        for s, z in enumerate(planes):
            for j in range(5):
                boxed = [three_along_x([stage_x[s, j, 3 * i + t] for t in range(3)], 3, lane) for i in range(3)]
                centre = pl.ds(HALO + j, 8, stride=5)
                tail = raw[4, HALO + z, centre, :]
                f = [raw[0, HALO + z, centre, :], raw[1, HALO + z, centre, :], tail]
                m = [raw[2, HALO + z, centre, :], raw[3, HALO + z, centre, :], pltpu.roll(tail, 64, 1)]
                for t in range(3):
                    slope = f[t] * boxed[0][t] + m[t] * boxed[1][t] - boxed[2][t]
                    for c in range(3):
                        weighted[c, t, j, z] = slope * grad[t, c, z, pl.ds(j, 8, stride=5), :]

    main_part(middle_items)

    for copy in local[6:]:
        copy.wait()
    grad[2] = jnp.concatenate([g_tail[...], jnp.zeros_like(g_tail)], axis=-1)

    def relay(part):
        if part < 2:
            y_copies[2 * part].wait_recv()
            y_copies[2 * part + 1].wait_recv()
        else:
            y_copies[4].wait_recv()
        for k in ((0,), (1,), (2, 3))[part]:
            start_strips(k)
        for k, h in LATER[part]:
            start_plane(k, h)

    @pl.when(is_low_mid | is_high_mid)
    def _():
        for part in range(3):
            relay(part)

    @pl.loop(0, 7)
    def _(step):
        wait_planes(step // 2, step % 2)
        main_part(step_items(step))

        for after_step in sorted(set(PASS_AFTER)):
            @pl.when(step == after_step)
            def _():
                for i, when in enumerate(PASS_AFTER):
                    if when == after_step:
                        pass_on(i)

        for part in range(3):
            @pl.when((step == RELAY_AFTER[part]) & jnp.logical_not(is_low_mid | is_high_mid))
            def _():
                relay(part)

        @pl.when(step == RELAY_AFTER[2])
        def _():
            own_windows(strip)

        @pl.when(step == 5)
        def _():
            wait_strips(0)
            wait_strips(1)
            edge_part(middle_items + step_items(0) + step_items(1) + step_items(2))

    wait_strips(2)
    wait_strips(3)
    edge_part(step_items(3) + step_items(4) + step_items(5) + step_items(6))

    @pl.loop(3, 7)
    def _(step):
        slope_planes((7 - step, 2 + step), False)

    wy = [spline_weights(j) for j in range(SPACING)]
    wz = [[-2.0 * SIM_WEIGHT * w for w in ws] for ws in wy]

    def add_plane(slots, z, value):
        for k in range(4):
            weight = wz[z % SPACING][k]
            if weight != 0.0:
                m = z // SPACING + k
                slots[m] = weight * value if slots[m] is None else slots[m] + weight * value

    for t in range(3):
        @pl.loop(0, 3)
        def _(c):
            for j in range(SPACING):
                slots = [None] * 5
                for z in range(1, PLANES - 1):
                    add_plane(slots, z, weighted[c, t, j, z])
                for m in range(5):
                    inner_sum[c, t, j, m] = slots[m]

    wait_planes(3, 1)
    main_part(step_items(7))
    edge_part(step_items(7), 2)
    slope_planes((0, PLANES - 1), True)

    for t in range(3):
        @pl.loop(0, 3)
        def _(c):
            slots = []
            for j in range(SPACING):
                parts = [inner_sum[c, t, j, m] for m in range(5)]
                add_plane(parts, 0, weighted[c, t, j, 0])
                add_plane(parts, PLANES - 1, weighted[c, t, j, PLANES - 1])
                slots.append(parts)
            for m in range(5):
                y = []
                for k in range(4):
                    total = wy[0][k] * slots[0][m]
                    for j in range(1, SPACING):
                        total = total + wy[j][k] * slots[j][m]
                    y.append(total)
                r0, r2, r3 = pltpu.roll(y[0], 7, 0), pltpu.roll(y[2], 1, 0), pltpu.roll(y[3], 2, 0)
                inner = (
                    jnp.where(row == 7, 0.0, r0) + y[1] + jnp.where(row == 0, 0.0, r2) + jnp.where(row < 2, 0.0, r3)
                )
                to_low = jnp.where(row == 7, r0, 0.0)
                to_high = jnp.where(row == 0, r2, 0.0) + jnp.where(row < 2, r3, 0.0)
                clip_low = jnp.where(row == 0, y[0], 0.0)
                clip_high = jnp.where(row == 7, y[2] + y[3] + pltpu.roll(y[3], 1, 0), 0.0)
                is_low = gy == 0
                base = pl.multiple_of(48 * m + 8 * c, 8)
                lanes = pl.ds(128 * t, 128)
                wide[pl.ds(base, 8), lanes] = inner + jnp.where(is_low, clip_low, clip_high)
                wide[pl.ds(pl.multiple_of(base + 24, 8), 8), lanes] = jnp.where(is_low, to_high, to_low)

    left = wide[...]
    high = left.astype(jnp.bfloat16)
    low = (left - high.astype(jnp.float32)).astype(jnp.bfloat16)

    def dot(a, b):
        return jnp.dot(a, b, preferred_element_type=jnp.float32)

    total = dot(high, bh[...]) + (dot(low, bh[...]) + dot(high, bl[...]))
    sums[...] = total.reshape(5, 2, 3, 8, 128)

    copies = [
        (0, sums.at[0, 0], from_next, before, 0),
        (0, sums.at[0, 1], from_next_side, before_side, 1),
        (1, sums.at[pl.ds(3, 2), 0], from_prev, after, 2),
        (1, sums.at[pl.ds(3, 2), 1], from_prev_side, after_side, 3),
    ]
    rdmas = [
        (
            direction,
            pltpu.make_async_remote_copy(
                src_ref=src, dst_ref=dst, send_sem=e_send.at[i], recv_sem=e_recv.at[i],
                device_id=target, device_id_type=MESH,
            ),
        )
        for direction, src, dst, target, i in copies
    ]
    side_copy = pltpu.make_async_remote_copy(
        src_ref=sums.at[pl.ds(1, 2), 1], dst_ref=from_side, send_sem=e_send.at[4], recv_sem=e_recv.at[4],
        device_id=side, device_id_type=MESH,
    )

    @pl.when(jnp.logical_not(is_first))
    def _():
        for direction, copy in rdmas:
            if direction == 0:
                copy.start()

    @pl.when(jnp.logical_not(is_last))
    def _():
        for direction, copy in rdmas:
            if direction == 1:
                copy.start()

    low_clip = jnp.where(is_first, 1.0, 0.0)
    high_clip = jnp.where(is_last, 1.0, 0.0)
    sums[1] = sums[1] + low_clip * sums[0]
    sums[2] = sums[2] + high_clip * (sums[3] + sums[4])
    side_copy.start()

    @pl.when(is_last)
    def _():
        from_next[...] = jnp.zeros_like(from_next)
        from_next_side[...] = jnp.zeros_like(from_next_side)

    @pl.when(is_first)
    def _():
        from_prev[...] = jnp.zeros_like(from_prev)
        from_prev_side[...] = jnp.zeros_like(from_prev_side)

    @pl.when(jnp.logical_not(is_last))
    def _():
        for direction, copy in rdmas:
            if direction == 0:
                copy.wait_recv()

    @pl.when(jnp.logical_not(is_first))
    def _():
        for direction, copy in rdmas:
            if direction == 1:
                copy.wait_recv()

    side_copy.wait_recv()
    first = sums[1, 0] + from_side[0] + from_prev[0] + from_prev_side[0]
    second = sums[2, 0] + from_side[1] + from_prev[1] + from_prev_side[1] + from_next[...] + from_next_side[...]
    out_ref[0] = first[:, :, :POINTS]
    out_ref[1] = second[:, :, :POINTS]

    for copy in y_copies:
        copy.wait_send()
    for k in range(4):
        @pl.when(sends_up)
        def _():
            plane_to_after(k, 0).wait_send()
            plane_to_after(k, 1).wait_send()
            strip_to_after(k).wait_send()

        @pl.when(sends_down)
        def _():
            plane_to_before(k, 0).wait_send()
            plane_to_before(k, 1).wait_send()
            strip_to_before(k).wait_send()

    if detour:
        @pl.when(is_first | is_last)
        def _():
            for i in range(len(DETOUR)):
                on_up(i).wait_send()

    side_copy.wait_send()

    @pl.when(jnp.logical_not(is_first))
    def _():
        for direction, copy in rdmas:
            if direction == 0:
                copy.wait_send()

    @pl.when(jnp.logical_not(is_last))
    def _():
        for direction, copy in rdmas:
            if direction == 1:
                copy.wait_send()


def local_gradient(depth, fixed_image, moving_image, moving_grad):
    high, low = basis_along_x()
    f32 = jnp.float32
    anywhere = pl.BlockSpec(memory_space=pl.ANY)
    dma = pltpu.SemaphoreType.DMA
    return pl.pallas_call(
        functools.partial(kernel, depth),
        out_shape=jax.ShapeDtypeStruct((2, 3, 8, POINTS), f32),
        in_specs=[anywhere] * 5,
        out_specs=pl.BlockSpec(memory_space=pltpu.VMEM),
        scratch_shapes=[
            pltpu.VMEM((5, RAW_PLANES, RAW_ROWS, 128), f32),
            pltpu.VMEM((PLANES, ROWS, 64), f32),
            pltpu.VMEM((PLANES, ROWS, 64), f32),
            pltpu.VMEM((3, 3, PLANES, ROWS, 128), f32),
            pltpu.VMEM((3, PLANES, ROWS, 64), f32),
            pltpu.VMEM((384, 128), jnp.bfloat16),
            pltpu.VMEM((384, 128), jnp.bfloat16),
            pltpu.VMEM((13, COEF_PLANES, RAW_ROWS, 128), f32),
            pltpu.VMEM((2, 13, 64, 128), f32),
            pltpu.VMEM((104, RAW_ROWS, 128), f32),
            pltpu.VMEM((104, RAW_ROWS, 128), f32),
            pltpu.VMEM((8, 5, 15, 8, 128), f32),
            pltpu.VMEM((8, 5, 15, 8, 128), f32),
            pltpu.VMEM((9, COEF_PLANES, COEF_ROWS, 128), f32),
            pltpu.VMEM((3, 3, 5, PLANES, 8, 128), f32),
            pltpu.VMEM((3, 3, 5, 5, 8, 128), f32),
            pltpu.VMEM((240, 384), f32),
            pltpu.VMEM((5, 2, 3, 8, 128), f32),
            pltpu.VMEM((4, 5, ROWS, 128), f32),
            pltpu.VMEM((3, 8, 128), f32),
            pltpu.VMEM((2, 3, 8, 128), f32),
            pltpu.VMEM((2, 3, 8, 128), f32),
            pltpu.VMEM((3, 8, 128), f32),
            pltpu.VMEM((2, 3, 8, 128), f32),
            dma((11,)),
            dma((5,)),
            dma((5,)),
            dma((2, 4, 2)),
            dma((2, 4, 2)),
            dma((2, 4)),
            dma((2, 4)),
            dma((4,)),
            dma((4,)),
            dma((5,)),
            dma((5,)),
        ],
        compiler_params=pltpu.CompilerParams(collective_id=0, has_side_effects=True, vmem_limit_bytes=56500000),
    )(fixed_image, moving_image, moving_grad, high, low)


def solution(mesh):
    in_specs = (P("gz", "gy", None), P("gz", "gy", None), P(None, "gz", "gy", None))
    out_specs = P("gz", None, "gy", None)
    body = functools.partial(local_gradient, mesh.shape["gz"])
    return jax.shard_map(body, mesh=mesh, in_specs=in_specs, out_specs=out_specs, check_vma=False)
```

```python
import functools

import jax
import jax.numpy as jnp
import numpy as np
from jax import lax
from jax.experimental import pallas as pl
from jax.experimental.pallas import tpu as pltpu
from jax.sharding import PartitionSpec as P

RADIUS = 4
SPACING = 5
EPS = 36.0
SIM_WEIGHT = 8.0
WINDOW = float((2 * RADIUS + 1) ** 3)
MESH = pl.DeviceIdType.MESH

PLANES = 10
ROWS = 40
NX = 320
POINTS = 64
HALO = 2 * RADIUS
RAW_PLANES = PLANES + 2 * HALO
RAW_ROWS = ROWS + 2 * HALO
COEF_PLANES = PLANES + 2 * RADIUS
COEF_ROWS = ROWS + 2 * RADIUS
PAIRS = (0, 8, 2, 6, 4)
DETOUR = (((2, 1), 1), ((3, 0), 0), ((3, 1), 0))
PASS_AFTER = (3, 4, 5)
RELAY_AFTER = (2, 3, 4)
LATER = ((), ((3, 1),), ())
ROUND = tuple(plane for plane, way in DETOUR)


def spline_weights(step):
    u = step / SPACING
    return (
        (1.0 - u) ** 3 / 6.0,
        (3.0 * u**3 - 6.0 * u**2 + 4.0) / 6.0,
        (-3.0 * u**3 + 3.0 * u**2 + 3.0 * u + 1.0) / 6.0,
        u**3 / 6.0,
    )


def basis_along_x():
    matrix = np.zeros((384, 128), np.float64)
    for x in range(NX):
        for k, weight in enumerate(spline_weights(x % SPACING)):
            point = min(max(x // SPACING - 1 + k, 0), POINTS - 1)
            matrix[x, point] += weight
    matrix = matrix.astype(np.float32)
    high = matrix.astype(jnp.bfloat16)
    low = (matrix - high.astype(np.float32)).astype(jnp.bfloat16)
    return high, low


def suffix_sums(values):
    sums = [values[-1]]
    for value in reversed(values[:-1]):
        sums.append(sums[-1] + value)
    return sums[::-1]


def prefix_sums(values):
    sums = [values[0]]
    for value in values[1:]:
        sums.append(sums[-1] + value)
    return sums


def windows_of_nine(values):
    count = len(values) - 8
    if count > 9:
        before = suffix_sums(values[:9])
        after = prefix_sums(values[9:])
        return [before[0]] + [before[i] + after[i - 1] for i in range(1, 9)] + [after[8]]
    common = values[count - 1]
    for value in values[count:9]:
        common = common + value
    before = suffix_sums(values[: count - 1])
    after = prefix_sums(values[9:])
    out = []
    for i in range(count):
        total = common
        if i < count - 1:
            total = total + before[i]
        if i > 0:
            total = total + after[i - 1]
        out.append(total)
    return out


def three_along_x(tiles, reach, lane):
    right = [pltpu.roll(tile, reach, 1) for tile in tiles]
    left = [pltpu.roll(tile, 128 - reach, 1) for tile in tiles]
    out = []
    for i in range(3):
        before = jnp.where(lane < reach, right[i - 1], right[i])
        after = jnp.where(lane >= 128 - reach, left[(i + 1) % 3], left[i])
        out.append(tiles[i] + before + after)
    return out


def kernel(
    depth, f_hbm, m_hbm, g_hbm, bh_hbm, bl_hbm, out_ref,
    raw, f_tail, m_tail, grad, g_tail, bh, bl, own_sum, halo_sum, zsum, ysum, stage_y, stage_x, coef, weighted, inner_sum, wide,
    sums, passing, from_next, from_prev, from_side, from_next_side, from_prev_side,
    local_sem, y_send, y_recv, z_send, z_recv, s_send, s_recv, hop_send, hop_recv, e_send, e_recv,
):
    gz = lax.axis_index("gz")
    gy = lax.axis_index("gy")
    other = 1 - gy
    is_first = gz == 0
    is_last = gz == depth - 1
    before = (jnp.maximum(gz - 1, 0), gy)
    after = (jnp.minimum(gz + 1, depth - 1), gy)
    before_side = (jnp.maximum(gz - 1, 0), other)
    after_side = (jnp.minimum(gz + 1, depth - 1), other)
    side = (gz, other)
    middle = depth // 2
    detour = depth >= 4 and len(DETOUR) > 0
    is_low_mid = (gz == middle - 1) if detour else (gz < 0)
    is_high_mid = (gz == middle) if detour else (gz < 0)

    local = []

    def bring(src, dst):
        copy = pltpu.make_async_copy(src, dst, local_sem.at[len(local)])
        copy.start()
        local.append(copy)

    own = pl.ds(HALO, PLANES)
    rows_own = pl.ds(HALO, ROWS)
    bring(f_hbm.at[:, :, pl.ds(256, 64)], f_tail)
    bring(m_hbm.at[:, :, pl.ds(256, 64)], m_tail)
    for t in range(2):
        bring(f_hbm.at[:, :, pl.ds(128 * t, 128)], raw.at[t, own, rows_own, :])
        bring(m_hbm.at[:, :, pl.ds(128 * t, 128)], raw.at[2 + t, own, rows_own, :])
    for t in range(2):
        bring(g_hbm.at[:, :, :, pl.ds(128 * t, 128)], grad.at[t])
    bring(g_hbm.at[:, :, :, pl.ds(256, 64)], g_tail)
    bring(bh_hbm, bh)
    bring(bl_hbm, bl)

    barrier = pltpu.get_barrier_semaphore()
    pl.semaphore_signal(barrier, inc=1, device_id=side, device_id_type=MESH)

    @pl.when(jnp.logical_not(is_first))
    def _():
        pl.semaphore_signal(barrier, inc=1, device_id=before, device_id_type=MESH)
        pl.semaphore_signal(barrier, inc=1, device_id=before_side, device_id_type=MESH)

    @pl.when(jnp.logical_not(is_last))
    def _():
        pl.semaphore_signal(barrier, inc=1, device_id=after, device_id_type=MESH)
        pl.semaphore_signal(barrier, inc=1, device_id=after_side, device_id_type=MESH)

    if detour:
        @pl.when(is_low_mid | is_high_mid)
        def _():
            for far_slab in (0, depth - 1):
                pl.semaphore_signal(barrier, inc=1, device_id=(far_slab, gy), device_id_type=MESH)

        @pl.when(is_first | is_last)
        def _():
            for far_slab in (middle - 1, middle):
                pl.semaphore_signal(barrier, inc=1, device_id=(far_slab, gy), device_id_type=MESH)

    lane = lax.broadcasted_iota(jnp.int32, (8, 128), 1)
    row = lax.broadcasted_iota(jnp.int32, (8, 128), 0)
    zero = jnp.zeros((8, 128), jnp.float32)
    low_half = lane < 64

    zero_row = pl.multiple_of(48 * gy, 8)
    strip_row = pl.multiple_of(48 - 48 * gy, 8)
    raw[:, :, pl.ds(zero_row, 8), :] = jnp.zeros((5, RAW_PLANES, 8, 128), jnp.float32)
    halo_sum[...] = jnp.zeros_like(halo_sum)
    main_row = pl.multiple_of(8 * gy, 8)
    edge_row = pl.multiple_of(40 - 40 * gy, 8)

    local[0].wait()
    local[1].wait()
    for z in range(PLANES):
        raw[4, HALO + z, HALO : HALO + ROWS, :] = jnp.concatenate([f_tail[z], m_tail[z]], axis=-1)
    for copy in local[2:6]:
        copy.wait()

    if detour:
        @pl.when(is_low_mid | is_high_mid)
        def _():
            pl.semaphore_wait(barrier, 7)

        @pl.when(jnp.logical_not(is_low_mid | is_high_mid))
        def _():
            pl.semaphore_wait(barrier, 5)
    else:
        @pl.when(is_first | is_last)
        def _():
            pl.semaphore_wait(barrier, 3)

        @pl.when(jnp.logical_not(is_first | is_last))
        def _():
            pl.semaphore_wait(barrier, 5)

    src_row = pl.multiple_of(40 - 32 * gy, 8)
    y_copies = []
    for i, first in enumerate(PAIRS):
        copy = pltpu.make_async_remote_copy(
            src_ref=raw.at[:, pl.ds(HALO + first, 2), pl.ds(src_row, 8), :],
            dst_ref=raw.at[:, pl.ds(HALO + first, 2), pl.ds(zero_row, 8), :],
            send_sem=y_send.at[i], recv_sem=y_recv.at[i], device_id=side, device_id_type=MESH,
        )
        copy.start()
        y_copies.append(copy)

    def plane_to_after(k, h):
        return pltpu.make_async_remote_copy(
            src_ref=raw.at[:, 17 - 2 * k - h, rows_own, :],
            dst_ref=raw.at[:, 7 - 2 * k - h, rows_own, :],
            send_sem=z_send.at[0, k, h], recv_sem=z_recv.at[0, k, h], device_id=after, device_id_type=MESH,
        )

    def plane_to_before(k, h):
        return pltpu.make_async_remote_copy(
            src_ref=raw.at[:, 8 + 2 * k + h, rows_own, :],
            dst_ref=raw.at[:, 18 + 2 * k + h, rows_own, :],
            send_sem=z_send.at[1, k, h], recv_sem=z_recv.at[1, k, h], device_id=before, device_id_type=MESH,
        )

    strip = pl.ds(strip_row, 8)

    def strip_to_after(k):
        return pltpu.make_async_remote_copy(
            src_ref=raw.at[:, pl.ds(16 - 2 * k, 2), strip, :],
            dst_ref=raw.at[:, pl.ds(6 - 2 * k, 2), strip, :],
            send_sem=s_send.at[0, k], recv_sem=s_recv.at[0, k], device_id=after, device_id_type=MESH,
        )

    def strip_to_before(k):
        return pltpu.make_async_remote_copy(
            src_ref=raw.at[:, pl.ds(8 + 2 * k, 2), strip, :],
            dst_ref=raw.at[:, pl.ds(18 + 2 * k, 2), strip, :],
            send_sem=s_send.at[1, k], recv_sem=s_recv.at[1, k], device_id=before, device_id_type=MESH,
        )

    def hop_up(i):
        (k, h), way = DETOUR[i]
        return pltpu.make_async_remote_copy(
            src_ref=raw.at[:, 17 - 2 * k - h, rows_own, :], dst_ref=passing.at[i],
            send_sem=z_send.at[0, k, h], recv_sem=hop_recv.at[i],
            device_id=((0, depth - 1)[way], gy), device_id_type=MESH,
        )

    def hop_down(i):
        (k, h), way = DETOUR[i]
        return pltpu.make_async_remote_copy(
            src_ref=raw.at[:, 8 + 2 * k + h, rows_own, :], dst_ref=passing.at[i],
            send_sem=z_send.at[1, k, h], recv_sem=hop_recv.at[i],
            device_id=((depth - 1, 0)[way], gy), device_id_type=MESH,
        )

    def on_up(i):
        (k, h), way = DETOUR[i]
        return pltpu.make_async_remote_copy(
            src_ref=passing.at[i], dst_ref=raw.at[:, 7 - 2 * k - h, rows_own, :],
            send_sem=hop_send.at[i], recv_sem=z_recv.at[0, k, h], device_id=(middle, gy), device_id_type=MESH,
        )

    def on_down(i):
        (k, h), way = DETOUR[i]
        return pltpu.make_async_remote_copy(
            src_ref=passing.at[i], dst_ref=raw.at[:, 18 + 2 * k + h, rows_own, :],
            send_sem=hop_send.at[i], recv_sem=z_recv.at[1, k, h], device_id=(middle - 1, gy), device_id_type=MESH,
        )

    sends_up = jnp.logical_not(is_last)
    sends_down = jnp.logical_not(is_first)

    def start_plane(k, h):
        goes_round = (k, h) in ROUND
        up = sends_up & jnp.logical_not(is_low_mid) if goes_round else sends_up
        down = sends_down & jnp.logical_not(is_high_mid) if goes_round else sends_down

        @pl.when(up)
        def _():
            plane_to_after(k, h).start()

        @pl.when(down)
        def _():
            plane_to_before(k, h).start()

    def start_strips(k):
        @pl.when(sends_up)
        def _():
            strip_to_after(k).start()

        @pl.when(sends_down)
        def _():
            strip_to_before(k).start()

    def start_hop(i):
        @pl.when(is_low_mid)
        def _():
            hop_up(i).start()

        @pl.when(is_high_mid)
        def _():
            hop_down(i).start()

    def pass_on(i):
        if detour and i < len(DETOUR):
            way = DETOUR[i][1]

            @pl.when((is_first, is_last)[way])
            def _():
                hop_up(i).wait_recv()
                on_up(i).start()

            @pl.when((is_last, is_first)[way])
            def _():
                hop_down(i).wait_recv()
                on_down(i).start()

    def wait_planes(k, h):
        @pl.when(sends_down)
        def _():
            plane_to_after(k, h).wait_recv()

        @pl.when(sends_up)
        def _():
            plane_to_before(k, h).wait_recv()

    def wait_strips(k):
        @pl.when(sends_down)
        def _():
            strip_to_after(k).wait_recv()

        @pl.when(sends_up)
        def _():
            strip_to_before(k).wait_recv()

    for k, h in ((0, 0), (0, 1), (1, 0), (1, 1), (2, 0), (2, 1), (3, 0), (3, 1)):
        if (k, h) < (3, 1):
            start_plane(k, h)
        if detour and (k, h) in ROUND:
            start_hop(ROUND.index((k, h)))

    @pl.when(is_first)
    def _():
        raw[:, 0:HALO, :, :] = jnp.zeros((5, HALO, RAW_ROWS, 128), jnp.float32)

    @pl.when(is_last)
    def _():
        raw[:, HALO + PLANES : RAW_PLANES, :, :] = jnp.zeros((5, HALO, RAW_ROWS, 128), jnp.float32)

    def fields_of(plane, rows):
        out = []
        for t in range(2):
            f = raw[t, plane, rows, :]
            m = raw[2 + t, plane, rows, :]
            out += [f, m, f * f, m * m, f * m]
        p = raw[4, plane, rows, :]
        return out + [p, p * p, p * pltpu.roll(p, 64, 1)]

    def own_windows(rows):
        columns = [fields_of(HALO + z, rows) for z in range(PLANES)]
        for col in range(13):
            values = [columns[z][col] for z in range(PLANES)]
            for p, total in enumerate(prefix_sums(values[:9])):
                own_sum[col, p, rows, :] = total
            for p, total in enumerate(suffix_sums(values[1:])):
                own_sum[col, 9 + p, rows, :] = total

    @pl.loop(0, 6)
    def _(i):
        own_windows(pl.ds(pl.multiple_of(main_row + 8 * i, 8), 8))

    def coefficients(items, base, count, part, first=0):
        offset = 48 * part
        for n, (plane, halo, side_of) in enumerate(items, first):
            for g in range(count + 1):
                rows = pl.ds(pl.multiple_of(base + 8 * g, 8), 8)
                here = pl.ds(8 * g, 8)
                if halo is None:
                    for col in range(13):
                        zsum[13 * n + col, here, :] = own_sum[col, plane, rows, :]
                else:
                    there = pl.ds(offset + 8 * g, 8)
                    fields = fields_of(halo, rows)
                    for col in range(13):
                        total = halo_sum[side_of, col, there, :] + fields[col]
                        halo_sum[side_of, col, there, :] = total
                        zsum[13 * n + col, here, :] = total + own_sum[col, plane, rows, :]
        for n in range(first, first + len(items)):
            for col in range(13):
                at = 13 * n + col
                for g in range(count + 1):
                    ysum[at, pl.ds(8 * g, 8), :] = (
                        zsum[at, pl.ds(8 * g, 8), :] + zsum[at, pl.ds(8 * g + 1, 8), :] + zsum[at, pl.ds(8 * g + 2, 8), :]
                    )
                for j in range(count):
                    total = (
                        ysum[at, pl.ds(8 * j, 8), :] + ysum[at, pl.ds(8 * j + 3, 8), :] + ysum[at, pl.ds(8 * j + 6, 8), :]
                    )
                    if col < 10:
                        stage_y[n, j, 3 * (col % 5) + col // 5] = total
                    elif col == 12:
                        stage_y[n, j, 14] = jnp.where(low_half, total, 0.0)
                    else:
                        stage_y[n, j, 6 * (col - 10) + 2] = jnp.where(low_half, total, 0.0)
                        stage_y[n, j, 6 * (col - 10) + 5] = jnp.where(low_half, pltpu.roll(total, 64, 1), 0.0)
        for n in range(first, first + len(items)):
            for j in range(count):
                for i in range(5):
                    three = three_along_x([stage_y[n, j, 3 * i + t] for t in range(3)], 1, lane)
                    for t in range(3):
                        stage_x[n, j, 3 * i + t] = three[t]
        for n, (plane, halo, side_of) in enumerate(items, first):
            position = gz * PLANES + plane - RADIUS
            inside = (position >= 0) & (position < depth * PLANES)
            for j in range(count):
                boxed = [three_along_x([stage_x[n, j, 3 * i + t] for t in range(3)], 3, lane) for i in range(5)]
                position = base + 8 * j + row + 40 * gy - RADIUS
                valid = jnp.where(inside & (position >= 0) & (position < 80), 1.0, 0.0)
                where = pl.ds(pl.multiple_of(base + 8 * j, 8), 8)
                for t in range(3):
                    sf, sm, sff, smm, sfm = [boxed[i][t] for i in range(5)]
                    mf = sf * (1.0 / WINDOW)
                    mm = sm * (1.0 / WINDOW)
                    a = (sfm - mf * sm) * (valid if t < 2 else jnp.where(low_half, valid, 0.0))
                    p = sff - mf * sf + EPS
                    q = smm - mm * sm + EPS
                    r = 1.0 / (p * q)
                    cross = a * r
                    moving = -cross * a * (r * p)
                    for i, value in enumerate((cross, moving, cross * mf + moving * mm)):
                        if halo is not None:
                            value = value + coef[3 * i + t, plane + (1, -1)[side_of], where, :]
                        coef[3 * i + t, plane, where, :] = value

    middle_items = [(8, None, 0), (9, None, 1)]

    def step_items(step):
        return [(7 - step, 7 - step, 0), (10 + step, 18 + step, 1)]

    def main_part(items):
        coefficients(items, main_row, 5, 0)

    def edge_part(items, first=0):
        coefficients(items, edge_row, 1, 1, first)

    def slope_planes(planes, ends):
        for s, z in enumerate(planes):
            for col in range(9):
                values = []
                for m in range(13):
                    where = pl.ds(m, 8, stride=5)
                    if ends:
                        values.append(coef[col, (0, COEF_PLANES - 1)[s], where, :])
                    else:
                        values.append(coef[col, z, where, :] + coef[col, z + 2 * RADIUS, where, :])
                total = windows_of_nine(values)
                for j in range(5):
                    stage_y[s, j, col] = total[j]
        for s in range(2):
            for j in range(5):
                for i in range(3):
                    three = three_along_x([stage_y[s, j, 3 * i + t] for t in range(3)], 1, lane)
                    for t in range(3):
                        stage_x[s, j, 3 * i + t] = three[t]
        for s, z in enumerate(planes):
            for j in range(5):
                boxed = [three_along_x([stage_x[s, j, 3 * i + t] for t in range(3)], 3, lane) for i in range(3)]
                centre = pl.ds(HALO + j, 8, stride=5)
                tail = raw[4, HALO + z, centre, :]
                f = [raw[0, HALO + z, centre, :], raw[1, HALO + z, centre, :], tail]
                m = [raw[2, HALO + z, centre, :], raw[3, HALO + z, centre, :], pltpu.roll(tail, 64, 1)]
                for t in range(3):
                    slope = f[t] * boxed[0][t] + m[t] * boxed[1][t] - boxed[2][t]
                    for c in range(3):
                        weighted[c, t, j, z] = slope * grad[t, c, z, pl.ds(j, 8, stride=5), :]

    main_part(middle_items)

    for copy in local[6:]:
        copy.wait()
    grad[2] = jnp.concatenate([g_tail[...], jnp.zeros_like(g_tail)], axis=-1)

    def relay(part):
        if part < 2:
            y_copies[2 * part].wait_recv()
            y_copies[2 * part + 1].wait_recv()
        else:
            y_copies[4].wait_recv()
        for k in ((0,), (1,), (2, 3))[part]:
            start_strips(k)
        for k, h in LATER[part]:
            start_plane(k, h)

    @pl.when(is_low_mid | is_high_mid)
    def _():
        for part in range(3):
            relay(part)

    @pl.loop(0, 7)
    def _(step):
        wait_planes(step // 2, step % 2)
        main_part(step_items(step))

        for after_step in sorted(set(PASS_AFTER)):
            @pl.when(step == after_step)
            def _():
                for i, when in enumerate(PASS_AFTER):
                    if when == after_step:
                        pass_on(i)

        for part in range(3):
            @pl.when((step == RELAY_AFTER[part]) & jnp.logical_not(is_low_mid | is_high_mid))
            def _():
                relay(part)

        @pl.when(step == RELAY_AFTER[2])
        def _():
            own_windows(strip)

        @pl.when(step == 5)
        def _():
            wait_strips(0)
            wait_strips(1)
            edge_part(middle_items + step_items(0) + step_items(1) + step_items(2))

    wait_strips(2)
    wait_strips(3)
    edge_part(step_items(3) + step_items(4) + step_items(5) + step_items(6))

    @pl.loop(3, 7)
    def _(step):
        slope_planes((7 - step, 2 + step), False)

    wy = [spline_weights(j) for j in range(SPACING)]
    wz = [[-2.0 * SIM_WEIGHT * w for w in ws] for ws in wy]

    def add_plane(slots, z, value):
        for k in range(4):
            weight = wz[z % SPACING][k]
            if weight != 0.0:
                m = z // SPACING + k
                slots[m] = weight * value if slots[m] is None else slots[m] + weight * value

    for t in range(3):
        @pl.loop(0, 3)
        def _(c):
            for j in range(SPACING):
                slots = [None] * 5
                for z in range(1, PLANES - 1):
                    add_plane(slots, z, weighted[c, t, j, z])
                for m in range(5):
                    inner_sum[c, t, j, m] = slots[m]

    wait_planes(3, 1)
    main_part(step_items(7))
    edge_part(step_items(7), 2)
    slope_planes((0, PLANES - 1), True)

    for t in range(3):
        @pl.loop(0, 3)
        def _(c):
            slots = []
            for j in range(SPACING):
                parts = [inner_sum[c, t, j, m] for m in range(5)]
                add_plane(parts, 0, weighted[c, t, j, 0])
                add_plane(parts, PLANES - 1, weighted[c, t, j, PLANES - 1])
                slots.append(parts)
            for m in range(5):
                y = []
                for k in range(4):
                    total = wy[0][k] * slots[0][m]
                    for j in range(1, SPACING):
                        total = total + wy[j][k] * slots[j][m]
                    y.append(total)
                r0, r2, r3 = pltpu.roll(y[0], 7, 0), pltpu.roll(y[2], 1, 0), pltpu.roll(y[3], 2, 0)
                inner = (
                    jnp.where(row == 7, 0.0, r0) + y[1] + jnp.where(row == 0, 0.0, r2) + jnp.where(row < 2, 0.0, r3)
                )
                to_low = jnp.where(row == 7, r0, 0.0)
                to_high = jnp.where(row == 0, r2, 0.0) + jnp.where(row < 2, r3, 0.0)
                clip_low = jnp.where(row == 0, y[0], 0.0)
                clip_high = jnp.where(row == 7, y[2] + y[3] + pltpu.roll(y[3], 1, 0), 0.0)
                is_low = gy == 0
                base = pl.multiple_of(48 * m + 8 * c, 8)
                lanes = pl.ds(128 * t, 128)
                wide[pl.ds(base, 8), lanes] = inner + jnp.where(is_low, clip_low, clip_high)
                wide[pl.ds(pl.multiple_of(base + 24, 8), 8), lanes] = jnp.where(is_low, to_high, to_low)

    left = wide[...]
    high = left.astype(jnp.bfloat16)
    low = (left - high.astype(jnp.float32)).astype(jnp.bfloat16)

    def dot(a, b):
        return jnp.dot(a, b, preferred_element_type=jnp.float32)

    total = dot(high, bh[...]) + (dot(low, bh[...]) + dot(high, bl[...]))
    sums[...] = total.reshape(5, 2, 3, 8, 128)

    copies = [
        (0, sums.at[0, 0], from_next, before, 0),
        (0, sums.at[0, 1], from_next_side, before_side, 1),
        (1, sums.at[pl.ds(3, 2), 0], from_prev, after, 2),
        (1, sums.at[pl.ds(3, 2), 1], from_prev_side, after_side, 3),
    ]
    rdmas = [
        (
            direction,
            pltpu.make_async_remote_copy(
                src_ref=src, dst_ref=dst, send_sem=e_send.at[i], recv_sem=e_recv.at[i],
                device_id=target, device_id_type=MESH,
            ),
        )
        for direction, src, dst, target, i in copies
    ]
    side_copy = pltpu.make_async_remote_copy(
        src_ref=sums.at[pl.ds(1, 2), 1], dst_ref=from_side, send_sem=e_send.at[4], recv_sem=e_recv.at[4],
        device_id=side, device_id_type=MESH,
    )

    @pl.when(jnp.logical_not(is_first))
    def _():
        for direction, copy in rdmas:
            if direction == 0:
                copy.start()

    @pl.when(jnp.logical_not(is_last))
    def _():
        for direction, copy in rdmas:
            if direction == 1:
                copy.start()

    low_clip = jnp.where(is_first, 1.0, 0.0)
    high_clip = jnp.where(is_last, 1.0, 0.0)
    sums[1] = sums[1] + low_clip * sums[0]
    sums[2] = sums[2] + high_clip * (sums[3] + sums[4])
    side_copy.start()

    @pl.when(is_last)
    def _():
        from_next[...] = jnp.zeros_like(from_next)
        from_next_side[...] = jnp.zeros_like(from_next_side)

    @pl.when(is_first)
    def _():
        from_prev[...] = jnp.zeros_like(from_prev)
        from_prev_side[...] = jnp.zeros_like(from_prev_side)

    @pl.when(jnp.logical_not(is_last))
    def _():
        for direction, copy in rdmas:
            if direction == 0:
                copy.wait_recv()

    @pl.when(jnp.logical_not(is_first))
    def _():
        for direction, copy in rdmas:
            if direction == 1:
                copy.wait_recv()

    side_copy.wait_recv()
    first = sums[1, 0] + from_side[0] + from_prev[0] + from_prev_side[0]
    second = sums[2, 0] + from_side[1] + from_prev[1] + from_prev_side[1] + from_next[...] + from_next_side[...]
    out_ref[0] = first[:, :, :POINTS]
    out_ref[1] = second[:, :, :POINTS]

    for copy in y_copies:
        copy.wait_send()
    for k in range(4):
        @pl.when(sends_up)
        def _():
            plane_to_after(k, 0).wait_send()
            plane_to_after(k, 1).wait_send()
            strip_to_after(k).wait_send()

        @pl.when(sends_down)
        def _():
            plane_to_before(k, 0).wait_send()
            plane_to_before(k, 1).wait_send()
            strip_to_before(k).wait_send()

    if detour:
        @pl.when(is_first | is_last)
        def _():
            for i in range(len(DETOUR)):
                on_up(i).wait_send()

    side_copy.wait_send()

    @pl.when(jnp.logical_not(is_first))
    def _():
        for direction, copy in rdmas:
            if direction == 0:
                copy.wait_send()

    @pl.when(jnp.logical_not(is_last))
    def _():
        for direction, copy in rdmas:
            if direction == 1:
                copy.wait_send()


def local_gradient(depth, fixed_image, moving_image, moving_grad):
    high, low = basis_along_x()
    f32 = jnp.float32
    anywhere = pl.BlockSpec(memory_space=pl.ANY)
    dma = pltpu.SemaphoreType.DMA
    return pl.pallas_call(
        functools.partial(kernel, depth),
        out_shape=jax.ShapeDtypeStruct((2, 3, 8, POINTS), f32),
        in_specs=[anywhere] * 5,
        out_specs=pl.BlockSpec(memory_space=pltpu.VMEM),
        scratch_shapes=[
            pltpu.VMEM((5, RAW_PLANES, RAW_ROWS, 128), f32),
            pltpu.VMEM((PLANES, ROWS, 64), f32),
            pltpu.VMEM((PLANES, ROWS, 64), f32),
            pltpu.VMEM((3, 3, PLANES, ROWS, 128), f32),
            pltpu.VMEM((3, PLANES, ROWS, 64), f32),
            pltpu.VMEM((384, 128), jnp.bfloat16),
            pltpu.VMEM((384, 128), jnp.bfloat16),
            pltpu.VMEM((13, COEF_PLANES, RAW_ROWS, 128), f32),
            pltpu.VMEM((2, 13, 64, 128), f32),
            pltpu.VMEM((104, RAW_ROWS, 128), f32),
            pltpu.VMEM((104, RAW_ROWS, 128), f32),
            pltpu.VMEM((8, 5, 15, 8, 128), f32),
            pltpu.VMEM((8, 5, 15, 8, 128), f32),
            pltpu.VMEM((9, COEF_PLANES, COEF_ROWS, 128), f32),
            pltpu.VMEM((3, 3, 5, PLANES, 8, 128), f32),
            pltpu.VMEM((3, 3, 5, 5, 8, 128), f32),
            pltpu.VMEM((240, 384), f32),
            pltpu.VMEM((5, 2, 3, 8, 128), f32),
            pltpu.VMEM((4, 5, ROWS, 128), f32),
            pltpu.VMEM((3, 8, 128), f32),
            pltpu.VMEM((2, 3, 8, 128), f32),
            pltpu.VMEM((2, 3, 8, 128), f32),
            pltpu.VMEM((3, 8, 128), f32),
            pltpu.VMEM((2, 3, 8, 128), f32),
            dma((11,)),
            dma((5,)),
            dma((5,)),
            dma((2, 4, 2)),
            dma((2, 4, 2)),
            dma((2, 4)),
            dma((2, 4)),
            dma((4,)),
            dma((4,)),
            dma((5,)),
            dma((5,)),
        ],
        compiler_params=pltpu.CompilerParams(collective_id=0, has_side_effects=True, vmem_limit_bytes=56500000),
    )(fixed_image, moving_image, moving_grad, high, low)


def solution(mesh):
    in_specs = (P("gz", "gy", None), P("gz", "gy", None), P(None, "gz", "gy", None))
    out_specs = P("gz", None, "gy", None)
    body = functools.partial(local_gradient, mesh.shape["gz"])
    return jax.shard_map(body, mesh=mesh, in_specs=in_specs, out_specs=out_specs, check_vma=False)
```
